32 devices in a mesh: blk: 16 (over z, x, core), pair: 2 (over y).
Axes of the slice: x: 2, y: 2, z: 4, core: 2. Of those that a mesh axis runs over, the one named last changes fastest.
Arguments:
- vertex: bfloat16 [16, 2048, 2048], P('blk', 'pair'), may hold values from -0.125 to 0.125
- left_phase: bfloat16 [16, 2048, 512], P('blk', 'pair'), may hold values from -6 to 6
- right_phase: bfloat16 [16, 2048, 512], P('blk'), may hold values from -6 to 6
- tiles: bfloat16 [64, 512, 512], P('blk'), may hold values from -0.25 to 0.25
- orders: int32 [16], P('blk'), may hold values from 512 to 2048, as said below
- momentum: int32 [512], replicated, may hold values from 0 to 63
- frequency: int32 [512], replicated, may hold values from 0 to 31
Outputs:
- suscept: bfloat16 [64, 512, 512], P('blk', 'pair')
- sigma: float32 [2048], P(('blk', 'pair'))
The draws below stay inside these ranges and needn't reach their ends.
Inputs may be any that keep to these rules, and one draw needn't show every extreme that they name: `orders`: every order is at least 512 and at most 2048; some walker has order exactly 2048.
All inputs are finite; a program needn't handle non-finite values.
Results may differ from the reference program's by a relative error of at most 0.0075.
Values may be sent and summed in bfloat16 or wider, within the bound.
A program may use at most 64 MiB of HBM per device.

```python
import math
import jax
import jax.numpy as jnp
from jax import lax

S = 512
KMAX = 2048
TILES_DEV = 4
NMOM = 64
NFREQ = 32
WALKERS = 16
TILES = 64
N_BLK = 16


def draw_orders(key, part):
    values = jax.random.randint(key, (WALKERS,), KMAX // 4, KMAX + 1)
    chosen = jax.random.randint(jax.random.fold_in(key, 7), (), 0, WALKERS)
    return values.at[chosen].set(KMAX).astype(jnp.int32)


def touch_ends(array, stream_key, smallest, largest):
    longest = array.shape.index(max(array.shape))
    spots = []
    for shift in (0, 1):
        where = [jax.random.randint(jax.random.fold_in(stream_key, axis), (), 0, length) for axis, length in enumerate(array.shape)]
        where[longest] = (where[longest] + shift) % array.shape[longest]
        spots.append(tuple(where))
    return array.at[spots[0]].set(smallest).at[spots[1]].set(largest)


def block_scale(own_key, extent, split, low, largest):
    def one(position, shards_of):
        heights = jax.random.uniform(jax.random.fold_in(jax.random.fold_in(own_key, 6), position), (shards_of,), jnp.float32, low / len(split), largest / len(split))
        return jnp.repeat(jnp.exp(heights), extent[position] // shards_of).reshape((-1,) + (1,) * (len(extent) - position - 1))

    loudness = one(*split[0])
    for cut in split[1:]:
        loudness = loudness * one(*cut)
    return loudness


def normal_values(rng, extent, width, limit, split=(), kind=jnp.bfloat16):
    gain = block_scale(rng, extent, split, -0.22, 0.18) if split else 1.0
    values = jax.random.normal(rng, extent, jnp.float32) * width * gain
    return jnp.minimum(jnp.maximum(values, -limit), limit).astype(kind)


def setup_inputs(seed: int = 0) -> dict:
    seeds = jax.random.split(jax.random.key(seed), 8)
    return {
        "vertex": normal_values(seeds[0], (WALKERS, KMAX, KMAX), KMAX ** -0.5, 0.125, ((0, 16), (1, 2))),
        "left_phase": normal_values(seeds[1], (WALKERS, KMAX, S), 1.0, 6.0, ((0, 16), (1, 2))),
        "right_phase": normal_values(seeds[2], (WALKERS, KMAX, S), 1.0, 6.0, ((0, 16),)),
        "tiles": normal_values(seeds[3], (TILES, S, S), S ** -0.5, 0.25, ((0, 16),)),
        "orders": draw_orders(jax.random.fold_in(seeds[7], 71), 0),
        "momentum": touch_ends(jax.random.randint(seeds[5], (S,), 0, NMOM), jax.random.fold_in(seeds[5], 1), 0, NMOM - 1).astype(jnp.int32),
        "frequency": touch_ends(jax.random.randint(seeds[6], (S,), 0, NFREQ), jax.random.fold_in(seeds[6], 1), 0, NFREQ - 1).astype(jnp.int32),
    }


def reference(vertex, left_phase, right_phase, tiles, orders, momentum, frequency):
    positions = jnp.arange(KMAX, dtype=jnp.int32)

    def one_walker(items):
        matrix, left, right, order = items
        live = positions < order
        masked = jnp.where(live[:, None] & live[None, :], matrix, jnp.zeros_like(matrix))
        carried = jnp.dot(masked, right, preferred_element_type=jnp.float32).astype(jnp.bfloat16)
        green = lax.dot_general(left, carried, (((0,), (0,)), ((), ())), preferred_element_type=jnp.float32)
        return (green / math.sqrt(KMAX)).astype(jnp.bfloat16)
    greens = lax.map(one_walker, (vertex, left_phase, right_phase, orders))
    grouped = tiles.reshape(N_BLK, TILES_DEV, S, S)
    onehot_mom = (momentum[:, None] == jnp.arange(NMOM, dtype=jnp.int32)[None, :]).astype(jnp.float32)
    onehot_freq = (frequency[:, None] == jnp.arange(NFREQ, dtype=jnp.int32)[None, :]).astype(jnp.float32)
    offsets = jnp.arange(-2, 3, dtype=jnp.int32)

    def one_block(number):
        window = jnp.take(greens, (number + offsets) % N_BLK, axis=0).astype(jnp.float32)
        block_tiles = grouped[number].astype(jnp.float32)
        inner = jnp.einsum('usa,tab->utsb', window, block_tiles).astype(jnp.bfloat16).astype(jnp.float32)
        chi = jnp.einsum('utsb,ucb->tsc', inner, window) / math.sqrt(S)
        summed = lax.optimization_barrier(jnp.sum(chi, axis=0))
        partial_value = jnp.dot(summed, onehot_freq, precision=lax.Precision.HIGHEST)
        cells = jnp.dot(onehot_mom.T, partial_value, precision=lax.Precision.HIGHEST)
        return (chi.astype(jnp.bfloat16), cells)
    chis, cells = lax.map(one_block, jnp.arange(N_BLK, dtype=jnp.int32))
    factor = 1.0 / math.sqrt(5.0 * TILES_DEV * N_BLK * S * S / (NMOM * NFREQ))
    sigma = (lax.optimization_barrier(jnp.sum(cells, axis=0)) * factor).reshape(-1)
    return (chis.reshape(TILES_DEV * N_BLK, S, S), sigma)
```

```python
import math

import jax
import jax.numpy as jnp
from jax import lax
from jax.experimental import pallas as pl
from jax.experimental.pallas import tpu as pltpu
from jax.sharding import PartitionSpec as P

NMOM = 64
NFREQ = 32
LANES = 128
SIZE = 128
SPLIT = 2
MESH = pl.DeviceIdType.MESH
OWN, PEER, ACROSS, RELAYED, FORWARDED = range(5)

FIRST, HOP, NEAR, STEP = 7.2, 1.7, 1.0, 1.41
INNER, CHI = 0.5, 0.25


def contract(a, b, dims, precision=None):
    return lax.dot_general(
        a, b, (dims, ((), ())), preferred_element_type=jnp.float32, precision=precision
    )


def plan(count):
    step = STEP * 8 / count
    half = count // 2
    quarter = count // 4
    arrive = {}
    for k in range(count):
        y = FIRST + step * (k + 1)
        arrive["y", k] = y
        arrive["x", k] = y + step + HOP
        arrive["z", k] = y + 2 * (step + HOP)
        arrive["p", k] = y + NEAR
        arrive["f", k] = arrive["z", k] + NEAR
    source = {OWN: "y", PEER: "p", ACROSS: "x", RELAYED: "z", FORWARDED: "f"}
    jobs = []
    for slot in range(5):
        s = source[slot]
        for part in range(2):
            jobs.append((arrive[s, half - 1], INNER, ("inner", slot, part), [(s, half - 1)], []))
        for part in range(2):
            jobs.append((arrive[s, half - 1], CHI, ("own", slot, part), [(s, half - 1)],
                         [("inner", slot, part)]))
        for h in range(2):
            k = half + quarter * (h + 1) - 1
            if slot < RELAYED and h == 0:
                continue
            for part in range(2):
                length = CHI if slot < RELAYED else CHI / 2
                jobs.append((arrive[s, k], length, ("rest", slot, h, part), [(s, k)],
                             [("inner", slot, part)]))
    jobs.append((arrive["y", 1] + 0.5, 0.4, ("tiles", 0), [("y", 1)], []))
    jobs.append((arrive["y", 1] + 2.5, 0.3, ("tiles", 1), [("y", 1)], [("tiles", 0)]))
    jobs.append((arrive["y", count - 1], 0.3, ("cells", OWN), [("y", count - 1)], [("tiles", 1)]))
    jobs.append((arrive["x", count - 1], 0.3, ("cells", ACROSS), [("x", count - 1)],
                 [("cells", OWN)]))
    jobs.append((arrive["x", count - 1], 0.3, ("sigma",), [("x", count - 1)], [("cells", ACROSS)]))
    urgent = {"tiles": 0, "cells": 1, "sigma": 1, "inner": 2, "own": 3, "rest": 3}
    waits = sorted((t, key) for key, t in arrive.items() if key[0] in "yxz")
    order, done, now = [], set(), 0.0
    taken = set()
    while waits or jobs:
        if waits and waits[0][0] <= now + 0.1:
            t, key = waits.pop(0)
            now = max(now, t)
            order.append(key)
            taken.add(key)
            continue
        ready = [j for j in jobs if j[0] <= now and all(d in done for d in j[4])
                 and all(w in taken or w[0] in "pf" for w in j[3])]
        if ready:
            job = min(ready, key=lambda j: (urgent[j[2][0]], j[0]))
            jobs.remove(job)
            for w in job[3]:
                order.append(("need",) + w)
            order.append(job[2])
            done.add(job[2])
            now += job[1]
            continue
        times = [j[0] for j in jobs if j[0] > now] + ([waits[0][0]] if waits else [])
        now = min(times)
    return order


def body(sizes, order_ref, mom_ref, freq_ref, vertex_hbm, left_hbm, right_hbm, tiles_hbm,
         out_ref, sigma_ref,
         vertex, left, right, tiles, carried, partial, sending, arrived, greens, inner, acc,
         chi, tile_sum, tile_send, tile_recv, back_send, back_recv, weight_own, weight_across,
         cells_ref, sig_send, sig_recv, load_sem, y_send, y_recv, x_send, x_recv, z_send, z_recv,
         p_send, p_recv, f_send, f_recv, w_send, t_send, t_recv, s_send, s_recv, o_sem, token):
    n_blk, n_pair, height, breadth, states, n_tiles = sizes
    count = n_blk * n_pair
    half = states // n_pair
    b = lax.axis_index("blk")
    p = lax.axis_index("pair")
    me = b * n_pair + p
    chip = b // 2
    core = lax.rem(b, 2)
    odd = lax.rem(chip, 2)
    step = 1 - 2 * odd
    across = (lax.rem(b + 2 * step + n_blk, n_blk), p)
    along = (lax.rem(b + 4 * step + n_blk, n_blk), p)
    back = (lax.rem(b - 4 * step + n_blk, n_blk), p)
    peer = (b + 1 - 2 * core, p)
    other = (b, 1 - p)
    forwards_across = lax.rem(odd + core, 2) == 0
    low_end = b < 4
    high_end = b >= n_blk - 4
    even = odd == 0
    wrap_send = jnp.logical_or(jnp.logical_and(even, high_end),
                               jnp.logical_and(jnp.logical_not(even), low_end))
    wrap_recv = jnp.logical_or(jnp.logical_and(even, low_end),
                               jnp.logical_and(jnp.logical_not(even), high_end))

    barrier = pltpu.get_barrier_semaphore()
    for device in (other, across, peer, along, back):
        pl.semaphore_signal(barrier, inc=1, device_id=device, device_id_type=MESH)

    pieces = 4
    block = height // pieces
    wide = states // SPLIT

    def load_right(h):
        cols = pl.ds(h * wide, wide)
        return pltpu.make_async_copy(right_hbm.at[0, :, cols], right.at[h], load_sem.at[h])

    load_right(0).start()
    load_vertex = []
    for i in range(pieces):
        rows = pl.ds(i * block, block)
        copy = pltpu.make_async_copy(vertex_hbm.at[0, rows], vertex.at[rows], load_sem.at[SPLIT + i])
        copy.start()
        load_vertex.append(copy)
    load_left = pltpu.make_async_copy(left_hbm.at[0], left, load_sem.at[SPLIT + pieces])
    load_left.start()
    for h in range(1, SPLIT):
        load_right(h).start()
    load_tiles = pltpu.make_async_copy(tiles_hbm, tiles, load_sem.at[SPLIT + 1 + pieces])
    load_tiles.start()

    order = order_ref[0]
    scale = 1.0 / math.sqrt(breadth)
    per = half // SIZE
    total = n_pair * SPLIT * per
    middle = total // 2

    def chunk(which, k):
        group, h, i = k // (SPLIT * per), k // per % SPLIT, k % per
        start = lax.rem(which + group, n_pair) * half + i * SIZE
        return pl.ds(pl.multiple_of(start, SIZE), SIZE), pl.ds(h * wide, wide)

    def remote(src, dst, send, recv, device):
        return pltpu.make_async_remote_copy(src_ref=src, dst_ref=dst, send_sem=send, recv_sem=recv,
                                            device_id=device, device_id_type=MESH)

    def exchange(k, which):
        rows = chunk(which, k)
        return remote(sending.at[*rows], arrived.at[*rows], y_send.at[k], y_recv.at[k], other)

    def hop(source, target, k, send, recv, device):
        rows = chunk(p, k)
        return remote(greens.at[source, *rows], greens.at[target, *rows], send, recv, device)

    def to_across(k):
        return hop(OWN, ACROSS, k, x_send.at[k], x_recv.at[k], across)

    def to_peer(k):
        return hop(OWN, PEER, k, p_send.at[k], p_recv.at[k], peer)

    def to_along(k):
        return hop(ACROSS, RELAYED, k, z_send.at[k], z_recv.at[k], along)

    def to_other(k):
        return hop(RELAYED, RELAYED, k, w_send.at[k], z_recv.at[k + middle], other)

    def forward(source, k):
        return hop(source, FORWARDED, k, f_send.at[k], f_recv.at[k], peer)

    def send_tiles():
        return remote(tile_send, tile_recv, t_send.at[0], t_recv.at[0], peer)

    def send_back():
        return remote(back_send, back_recv, t_send.at[1], t_recv.at[1], back)

    ring = n_blk // 4
    rounds = 3 + max(ring // 2 - 1, 0)

    def near(r):
        return (other, across, peer) if r < 3 else (along, back)

    def give(r):
        for device in near(r):
            pl.semaphore_signal(token.at[r], inc=1, device_id=device, device_id_type=MESH)

    def take(r):
        pl.semaphore_wait(token.at[r], len(near(r)))

    def mask_right(h):
        def part(i, carry):
            rows = pl.ds(pl.multiple_of(i * 256, 256), 256)
            ids = i * 256 + lax.broadcasted_iota(jnp.int32, (256, wide), 0)
            right[h, rows, :] = jnp.where(ids < order, right[h, rows, :],
                                          jnp.zeros((), jnp.bfloat16))
            return carry

        lax.fori_loop(0, breadth // 256, part, 0)

    def carry_half(h):
        for i in range(pieces):
            rows = pl.ds(i * block, block)
            if h == 0:
                load_vertex[i].wait()
            product = contract(vertex[rows, :], right[h], ((1,), (0,)))
            ids = p * height + i * block + lax.broadcasted_iota(jnp.int32, (block, wide), 0)
            carried[h, rows, :] = jnp.where(ids < order, product, 0.0).astype(jnp.bfloat16)

    def partial_block(group, h):
        which = lax.rem(1 - p + group, n_pair)
        rows = pl.ds(pl.multiple_of(which * half, half), half)
        cols = pl.ds(h * wide, wide)
        product = contract(left[:, rows], carried[h], ((0,), (0,))) * scale
        partial[rows, cols] = product
        sending[rows, cols] = product.astype(jnp.bfloat16)
        for i in range(per):
            exchange((group * SPLIT + h) * per + i, 1 - p).start()

    load_right(0).wait()
    mask_right(0)
    carry_half(0)
    load_left.wait()
    pl.semaphore_wait(barrier, 5)
    partial_block(0, 0)
    give(0)
    for h in range(1, SPLIT):
        load_right(h).wait()
        mask_right(h)
        carry_half(h)
        partial_block(0, h)
    for group in range(1, n_pair):
        for h in range(SPLIT):
            partial_block(group, h)

    ids_m = lax.broadcasted_iota(jnp.int32, (NMOM, states), 0)
    pick_mom = (ids_m == mom_ref[...]).astype(jnp.bfloat16)
    ids_f = lax.broadcasted_iota(jnp.int32, (LANES, states), 0)
    pick_freq = (ids_f == freq_ref[...]).astype(jnp.bfloat16)
    own_rows = pl.ds(pl.multiple_of(p * half, half), half)
    rest_rows = pl.ds(pl.multiple_of((1 - p) * half, half), half)
    out_scale = 1.0 / math.sqrt(states)
    pair_share = forwards_across.astype(jnp.float32)

    load_tiles.wait()

    def tile_stage(stage):
        if stage == 0:
            value = tiles[0, own_rows, :].astype(jnp.float32)
            for t in range(1, n_tiles):
                value = value + tiles[t, own_rows, :].astype(jnp.float32)
            tile_sum[...] = value
            tile_send[...] = value.astype(jnp.bfloat16)
            send_tiles().start()
        else:
            send_tiles().wait_recv()
            mine = tile_sum[...]
            theirs = tile_recv[...].astype(jnp.float32)
            back_send[...] = (mine + (1.0 - pair_share) * theirs).astype(jnp.bfloat16)
            send_back().start()
            weight_own[...] = (mine + theirs).astype(jnp.bfloat16)
            tile_sum[...] = mine + pair_share * theirs

    def cells(slot):
        if slot == ACROSS:
            send_back().wait_recv()
            weight_across[...] = (
                tile_sum[...] + back_recv[...].astype(jnp.float32)
            ).astype(jnp.bfloat16)
        weight = weight_own if slot == OWN else weight_across
        folded = contract(pick_mom, greens[slot], ((1,), (0,)))
        folded = jnp.where(p == 0, folded[:, :half], folded[:, half:])
        high = folded.astype(jnp.bfloat16)
        low = (folded - high.astype(jnp.float32)).astype(jnp.bfloat16)
        joined = (contract(high, weight[...], ((1,), (0,)))
                  + contract(low, weight[...], ((1,), (0,))))
        picked = contract(pick_freq, greens[slot], ((1,), (0,)))
        value = contract(joined, picked, ((1,), (1,)), lax.Precision.HIGHEST)
        cells_ref[...] = value if slot == OWN else cells_ref[...] + value

    own_cells = NMOM * NFREQ // count

    def owner(i):
        to = lax.rem(me + i, count)
        return remote(sig_send.at[to], sig_recv.at[i - 1], s_send.at[i - 1], s_recv.at[i - 1],
                      (to // n_pair, lax.rem(to, n_pair)))

    def sigma():
        value_cells = cells_ref[...]
        rows_d = lax.broadcasted_iota(jnp.int32, (count, NMOM), 0)
        cols_m = lax.broadcasted_iota(jnp.int32, (count, NMOM), 1)
        spread = jnp.zeros((count, LANES), jnp.float32)
        if own_cells >= NFREQ:
            group = own_cells // NFREQ
            for k in range(group):
                pick = (cols_m == rows_d * group + k).astype(jnp.float32)
                value = contract(pick, value_cells, ((1,), (0,)), lax.Precision.HIGHEST)
                spread = spread + (pltpu.roll(value, NFREQ * k, 1) if k else value)
        else:
            group = NFREQ // own_cells
            for k in range(group):
                pick = (rows_d == cols_m * group + k).astype(jnp.float32)
                value = contract(pick, value_cells, ((1,), (0,)), lax.Precision.HIGHEST)
                spread = spread + (pltpu.roll(value, LANES - own_cells * k, 1) if k else value)
        factor = 1.0 / math.sqrt(5.0 * n_tiles * n_blk * states * states / (NMOM * NFREQ))
        sig_send[...] = (spread * (factor * out_scale)).reshape(count, 1, LANES)

        def send_cells(i, carry):
            owner(i).start()
            return carry

        lax.fori_loop(1, count, send_cells, 0)

    share = n_tiles // 2

    def compute_inner(slot, part):
        upper = greens[slot, own_rows, :]
        for t in range(part * share, (part + 1) * share):
            inner[slot, pl.ds(t * half, half), :] = contract(
                upper, tiles[t], ((1,), (0,))).astype(jnp.bfloat16)

    started = set()
    pending = {(0, part): 5 for part in range(2)} | {(1, part): 7 for part in range(2)}

    def store(group, t):
        rows = own_rows if group == 0 else rest_rows
        return pltpu.make_async_copy(chi.at[group, t], out_ref.at[t, :, rows],
                                     o_sem.at[group, t])

    def compute_chi(group, slot, part, k_half=None):
        rows = own_rows if group == 0 else rest_rows
        cols = pl.ds(0, states) if k_half is None else pl.ds(k_half * wide, wide)
        first = (group, part) not in started
        started.add((group, part))
        pending[group, part] -= 1
        last = pending[group, part] == 0
        for t in range(part * share, (part + 1) * share):
            lines = pl.ds(t * half, half)
            value = contract(inner[slot, lines, cols], greens[slot, rows, cols], ((1,), (1,)))
            if not first:
                value = acc[group, lines, :] + value
            if last:
                chi[group, t] = (value * out_scale).astype(jnp.bfloat16)
                store(group, t).start()
            else:
                acc[group, lines, :] = value

    def take_y(k):
        rows = chunk(p, k)
        exchange(k, p).wait_recv()
        greens[OWN, *rows] = (
            partial[*rows] + arrived[*rows].astype(jnp.float32)
        ).astype(jnp.bfloat16)
        to_across(k).start()
        to_peer(k).start()

    def take_x(k):
        to_across(k).wait_recv()
        if k < middle:
            to_along(k).start()
        else:
            @pl.when(jnp.logical_not(wrap_send))
            def _():
                to_along(k).start()

        @pl.when(forwards_across)
        def _():
            forward(ACROSS, k).start()

    def take_z(k):
        to_along(k).wait_recv()
        if k < middle:
            @pl.when(wrap_recv)
            def _():
                to_other(k).start()

        @pl.when(jnp.logical_not(forwards_across))
        def _():
            forward(RELAYED, k).start()

    waited = {"p": 0, "f": 0}

    def need(kind, k):
        if kind in waited:
            while waited[kind] <= k:
                at = waited[kind]
                (to_peer(at) if kind == "p" else forward(ACROSS, at)).wait_recv()
                waited[kind] += 1

    passed = 0
    for task in plan(total):
        kind = task[0]
        if kind == "y":
            take_y(task[1])
        elif kind == "x":
            take_x(task[1])
            if passed < rounds - 1:
                take(passed)
                passed += 1
                give(passed)
        elif kind == "z":
            take_z(task[1])
        elif kind == "need":
            need(task[1], task[2])
        elif kind == "tiles":
            tile_stage(task[1])
        elif kind == "cells":
            cells(task[1])
        elif kind == "sigma":
            while passed < rounds - 1:
                take(passed)
                passed += 1
                give(passed)
            take(passed)
            sigma()
        elif kind == "inner":
            compute_inner(task[1], task[2])
        elif kind == "own":
            compute_chi(0, task[1], task[2])
        elif kind == "rest":
            compute_chi(1, task[1], task[3], None if task[1] < RELAYED else task[2])

    for k in range(total):
        exchange(k, 1 - p).wait_send()
        to_across(k).wait_send()
        to_peer(k).wait_send()
        forward(ACROSS, k).wait_send()
        if k < middle:
            to_along(k).wait_send()

            @pl.when(wrap_recv)
            def _():
                to_other(k).wait_send()
        else:
            @pl.when(jnp.logical_not(wrap_send))
            def _():
                to_along(k).wait_send()
    send_tiles().wait_send()
    send_back().wait_send()

    def take_cells(i, carry):
        owner(i).wait()
        return carry

    lax.fori_loop(1, count, take_cells, 0)
    summed = jnp.sum(sig_recv[...], axis=0) + sig_send[me]
    sigma_ref[...] = summed[:, :own_cells]
    for group in range(2):
        for t in range(n_tiles):
            store(group, t).wait()


def solution(mesh):
    n_blk, n_pair = mesh.shape["blk"], mesh.shape["pair"]
    count = n_blk * n_pair

    def per_device(vertex, left_phase, right_phase, tiles, orders, momentum, frequency):
        height, breadth = vertex.shape[1], vertex.shape[2]
        states = right_phase.shape[2]
        n_tiles = tiles.shape[0]
        half = states // n_pair
        sizes = (n_blk, n_pair, height, breadth, states, n_tiles)
        bf16, f32 = jnp.bfloat16, jnp.float32
        dma = pltpu.SemaphoreType.DMA
        chunks = n_pair * SPLIT * (half // SIZE)
        rounds = 3 + max(n_blk // 4 // 2 - 1, 0)
        chi, cells = pl.pallas_call(
            lambda *refs: body(sizes, *refs),
            out_shape=(
                jax.ShapeDtypeStruct((n_tiles, half, states), bf16),
                jax.ShapeDtypeStruct((1, NMOM * NFREQ // count), f32),
            ),
            in_specs=[
                pl.BlockSpec(memory_space=pltpu.SMEM),
                pl.BlockSpec(memory_space=pltpu.VMEM),
                pl.BlockSpec(memory_space=pltpu.VMEM),
            ] + [pl.BlockSpec(memory_space=pltpu.HBM)] * 4,
            out_specs=(
                pl.BlockSpec(memory_space=pltpu.HBM),
                pl.BlockSpec(memory_space=pltpu.VMEM),
            ),
            scratch_shapes=[
                pltpu.VMEM((height, breadth), bf16),
                pltpu.VMEM((height, states), bf16),
                pltpu.VMEM((SPLIT, breadth, states // SPLIT), bf16),
                pltpu.VMEM((n_tiles, states, states), bf16),
                pltpu.VMEM((SPLIT, height, states // SPLIT), bf16),
                pltpu.VMEM((states, states), f32),
                pltpu.VMEM((states, states), bf16),
                pltpu.VMEM((states, states), bf16),
                pltpu.VMEM((5, states, states), bf16),
                pltpu.VMEM((5, n_tiles * half, states), bf16),
                pltpu.VMEM((2, n_tiles * half, half), f32),
                pltpu.VMEM((2, n_tiles, half, half), bf16),
                pltpu.VMEM((half, states), f32),
            ] + [pltpu.VMEM((half, states), bf16)] * 6 + [
                pltpu.VMEM((NMOM, LANES), f32),
                pltpu.VMEM((count, 1, LANES), f32),
                pltpu.VMEM((count - 1, 1, LANES), f32),
                dma((SPLIT + 6,)),
            ] + [dma((chunks,))] * 11 + [dma((2,))] * 2 + [dma((count - 1,))] * 2 + [
                dma((2, n_tiles)), pltpu.SemaphoreType.REGULAR((rounds,))],
            compiler_params=pltpu.CompilerParams(
                collective_id=0, has_side_effects=True, vmem_limit_bytes=60 * 1024 * 1024
            ),
            name="measure_green",
        )(
            orders,
            momentum.reshape(1, states),
            frequency.reshape(1, states),
            vertex,
            left_phase,
            right_phase,
            tiles,
        )
        return chi, cells.reshape(-1)

    in_specs = (
        P("blk", "pair", None),
        P("blk", "pair", None),
        P("blk", None, None),
        P("blk", None, None),
        P("blk"),
        P(),
        P(),
    )
    out_specs = (P("blk", "pair", None), P(("blk", "pair")))
    return jax.shard_map(
        per_device, mesh=mesh, in_specs=in_specs, out_specs=out_specs, check_vma=False
    )
```

```python
import math

import jax
import jax.numpy as jnp
from jax import lax
from jax.experimental import pallas as pl
from jax.experimental.pallas import tpu as pltpu
from jax.sharding import PartitionSpec as P

NMOM = 64
NFREQ = 32
LANES = 128
SIZE = 128
SPLIT = 2
PIECES = 8
MESH = pl.DeviceIdType.MESH
OWN, PEER, ACROSS, RELAYED, FORWARDED = range(5)

FIRST, HOP, NEAR, STEP = 7.2, 1.7, 1.0, 1.41
INNER, CHI = 0.5, 0.25


def contract(a, b, dims, precision=None):
    return lax.dot_general(
        a, b, (dims, ((), ())), preferred_element_type=jnp.float32, precision=precision
    )


def plan(count):
    step = STEP * 8 / count
    half = count // 2
    quarter = count // 4
    arrive = {}
    for k in range(count):
        y = FIRST + step * (k + 1)
        arrive["y", k] = y
        arrive["x", k] = y + step + HOP
        arrive["z", k] = y + 2 * (step + HOP)
        arrive["p", k] = y + NEAR
        arrive["f", k] = arrive["z", k] + NEAR
    source = {OWN: "y", PEER: "p", ACROSS: "x", RELAYED: "z", FORWARDED: "f"}
    jobs = []
    for slot in range(5):
        s = source[slot]
        for part in range(2):
            jobs.append((arrive[s, half - 1], INNER, ("inner", slot, part), [(s, half - 1)], []))
        for part in range(2):
            jobs.append((arrive[s, half - 1], CHI, ("own", slot, part), [(s, half - 1)],
                         [("inner", slot, part)]))
        for h in range(2):
            k = half + quarter * (h + 1) - 1
            if slot < RELAYED and h == 0:
                continue
            for part in range(2):
                length = CHI if slot < RELAYED else CHI / 2
                jobs.append((arrive[s, k], length, ("rest", slot, h, part), [(s, k)],
                             [("inner", slot, part)]))
    jobs.append((arrive["y", count - 1], 0.3, ("cells", OWN), [("y", count - 1)], []))
    jobs.append((arrive["x", count - 1], 0.3, ("cells", ACROSS), [("x", count - 1)],
                 [("cells", OWN)]))
    jobs.append((arrive["x", count - 1], 0.3, ("sigma",), [("x", count - 1)], [("cells", ACROSS)]))
    urgent = {"cells": 1, "sigma": 1, "inner": 2, "own": 3, "rest": 3}
    waits = sorted((t, key) for key, t in arrive.items() if key[0] in "yxz")
    order, done, now = [], set(), 0.0
    taken = set()
    while waits or jobs:
        if waits and waits[0][0] <= now + 0.1:
            t, key = waits.pop(0)
            now = max(now, t)
            order.append(key)
            taken.add(key)
            continue
        ready = [j for j in jobs if j[0] <= now and all(d in done for d in j[4])
                 and all(w in taken or w[0] in "pf" for w in j[3])]
        if ready:
            job = min(ready, key=lambda j: (urgent[j[2][0]], j[0]))
            jobs.remove(job)
            for w in job[3]:
                order.append(("need",) + w)
            order.append(job[2])
            done.add(job[2])
            now += job[1]
            continue
        times = [j[0] for j in jobs if j[0] > now] + ([waits[0][0]] if waits else [])
        now = min(times)
    return order


def body(sizes, order_hbm, mom_hbm, freq_hbm, vertex_hbm, left_hbm, right_hbm, tiles_hbm,
         out_ref, sigma_ref,
         order_ref, mom_ref, freq_ref, small_sem, vertex, left, turned, right, tiles, carried, partial, sending, arrived, greens, inner, acc,
         tile_sum, tile_send, tile_recv, back_send, back_recv, weight_own, weight_across,
         cells_ref, sig_send, sig_recv, load_sem, y_send, y_recv, x_send, x_recv, z_send, z_recv,
         p_send, p_recv, f_send, f_recv, w_send, t_send, t_recv, s_send, s_recv, token):
    n_blk, n_pair, height, breadth, states, n_tiles = sizes
    count = n_blk * n_pair
    half = states // n_pair
    b = lax.axis_index("blk")
    p = lax.axis_index("pair")
    me = b * n_pair + p
    chip = b // 2
    core = lax.rem(b, 2)
    odd = lax.rem(chip, 2)
    step = 1 - 2 * odd
    across = (lax.rem(b + 2 * step + n_blk, n_blk), p)
    along = (lax.rem(b + 4 * step + n_blk, n_blk), p)
    back = (lax.rem(b - 4 * step + n_blk, n_blk), p)
    peer = (b + 1 - 2 * core, p)
    other = (b, 1 - p)
    forwards_across = lax.rem(odd + core, 2) == 0
    low_end = b < 4
    high_end = b >= n_blk - 4
    even = odd == 0
    wrap_send = jnp.logical_or(jnp.logical_and(even, high_end),
                               jnp.logical_and(jnp.logical_not(even), low_end))
    wrap_recv = jnp.logical_or(jnp.logical_and(even, low_end),
                               jnp.logical_and(jnp.logical_not(even), high_end))

    barrier = pltpu.get_barrier_semaphore()

    def tell(semaphore, devices):
        for device in devices:
            pl.semaphore_signal(semaphore, inc=1, device_id=device, device_id_type=MESH)

    def tell_column(semaphore):
        @pl.when(jnp.logical_not(wrap_send))
        def _():
            tell(semaphore, (along,))

        @pl.when(jnp.logical_not(wrap_recv))
        def _():
            tell(semaphore, (back,))

    beside = 2 - wrap_send.astype(jnp.int32) - wrap_recv.astype(jnp.int32)
    tell(barrier, (other, across, peer))
    tell_column(barrier)

    pieces = PIECES
    block = height // pieces
    wide = states // SPLIT

    def load_right(h):
        cols = pl.ds(h * wide, wide)
        return pltpu.make_async_copy(right_hbm.at[0, :, cols], right.at[h], load_sem.at[h])

    small = [
        pltpu.make_async_copy(order_hbm, order_ref, small_sem.at[0]),
        pltpu.make_async_copy(mom_hbm, mom_ref, small_sem.at[1]),
        pltpu.make_async_copy(freq_hbm, freq_ref, small_sem.at[2]),
    ]
    load_left = pltpu.make_async_copy(left_hbm.at[0], left, load_sem.at[SPLIT + pieces])
    load_tiles = pltpu.make_async_copy(tiles_hbm, tiles, load_sem.at[SPLIT + 1 + pieces])
    load_vertex = []
    for i in range(pieces):
        rows = pl.ds(i * block, block)
        load_vertex.append(
            pltpu.make_async_copy(vertex_hbm.at[0, rows], vertex.at[rows], load_sem.at[SPLIT + i]))
    small[0].start()
    load_left.start()
    load_right(0).start()
    for copy in load_vertex:
        copy.start()
    for copy in small[1:]:
        copy.start()

    scale = 1.0 / math.sqrt(breadth)
    per = half // SIZE
    total = n_pair * SPLIT * per
    middle = total // 2

    def chunk(which, k):
        group, h, i = k // (SPLIT * per), k // per % SPLIT, k % per
        start = lax.rem(which + group, n_pair) * half + i * SIZE
        return pl.ds(pl.multiple_of(start, SIZE), SIZE), pl.ds(h * wide, wide)

    def remote(src, dst, send, recv, device):
        return pltpu.make_async_remote_copy(src_ref=src, dst_ref=dst, send_sem=send, recv_sem=recv,
                                            device_id=device, device_id_type=MESH)

    def exchange(k, which):
        rows = chunk(which, k)
        return remote(sending.at[*rows], arrived.at[*rows], y_send.at[k], y_recv.at[k], other)

    def hop(source, target, k, send, recv, device):
        rows = chunk(p, k)
        return remote(greens.at[source, *rows], greens.at[target, *rows], send, recv, device)

    def to_across(k):
        return hop(OWN, ACROSS, k, x_send.at[k], x_recv.at[k], across)

    def to_peer(k):
        return hop(OWN, PEER, k, p_send.at[k], p_recv.at[k], peer)

    def to_along(k):
        return hop(ACROSS, RELAYED, k, z_send.at[k], z_recv.at[k], along)

    def to_other(k):
        return hop(RELAYED, RELAYED, k, w_send.at[k], z_recv.at[k + middle], other)

    def forward(source, k):
        return hop(source, FORWARDED, k, f_send.at[k], f_recv.at[k], peer)

    def send_tiles():
        return remote(tile_send, tile_recv, t_send.at[0], t_recv.at[0], peer)

    def send_back():
        return remote(back_send, back_recv, t_send.at[1], t_recv.at[1], back)

    column = max(n_blk // 4 - 2, 0)
    rounds = column + 2

    def give(r):
        if r < column:
            tell_column(token.at[r])
        else:
            tell(token.at[r], (other, across, peer))

    def take(r):
        pl.semaphore_wait(token.at[r], beside if r < column else 3)

    def mask_right(h):
        def part(i, carry):
            rows = pl.ds(pl.multiple_of(i * 256, 256), 256)
            ids = i * 256 + lax.broadcasted_iota(jnp.int32, (256, wide), 0)
            right[h, rows, :] = jnp.where(ids < order, right[h, rows, :],
                                          jnp.zeros((), jnp.bfloat16))
            return carry

        lax.fori_loop(0, breadth // 256, part, 0)

    def carry_half(h):
        for i in range(pieces):
            rows = pl.ds(i * block, block)
            if h == 0:
                load_vertex[i].wait()
                if i == pieces // 2:
                    load_right(1).start()
                    load_tiles.start()
            product = contract(vertex[rows, :], right[h], ((1,), (0,)))
            ids = p * height + i * block + lax.broadcasted_iota(jnp.int32, (block, wide), 0)
            carried[h, rows, :] = jnp.where(ids < order, product, 0.0).astype(jnp.bfloat16)

    def partial_block(group, h):
        which = lax.rem(1 - p + group, n_pair)
        rows = pl.ds(pl.multiple_of(which * half, half), half)
        cols = pl.ds(h * wide, wide)
        product = contract(turned[group], carried[h], ((1,), (0,))) * scale
        partial[rows, cols] = product
        sending[rows, cols] = product.astype(jnp.bfloat16)
        for i in range(per):
            exchange((group * SPLIT + h) * per + i, 1 - p).start()

    def turn(group):
        which = lax.rem(1 - p + group, n_pair)
        cols = pl.ds(pl.multiple_of(which * half, half), half)
        turned[group] = left[:, cols].T

    own_rows = pl.ds(pl.multiple_of(p * half, half), half)
    rest_rows = pl.ds(pl.multiple_of((1 - p) * half, half), half)
    out_scale = 1.0 / math.sqrt(states)
    pair_share = forwards_across.astype(jnp.float32)

    def tile_stage(stage):
        if stage == 0:
            value = tiles[0, own_rows, :].astype(jnp.float32)
            for t in range(1, n_tiles):
                value = value + tiles[t, own_rows, :].astype(jnp.float32)
            tile_sum[...] = value
            tile_send[...] = value.astype(jnp.bfloat16)
            send_tiles().start()
        else:
            send_tiles().wait_recv()
            mine = tile_sum[...]
            theirs = tile_recv[...].astype(jnp.float32)
            back_send[...] = (mine + (1.0 - pair_share) * theirs).astype(jnp.bfloat16)
            send_back().start()
            weight_own[...] = (mine + theirs).astype(jnp.bfloat16)
            tile_sum[...] = mine + pair_share * theirs

    small[0].wait()
    order = order_ref[0]
    load_left.wait()
    turn(0)
    load_right(0).wait()
    mask_right(0)
    carry_half(0)
    pl.semaphore_wait(barrier, 3 + beside)
    partial_block(0, 0)
    passed = 0
    give(passed)
    load_tiles.wait()
    tile_stage(0)
    for h in range(1, SPLIT):
        load_right(h).wait()
        mask_right(h)
        carry_half(h)
        partial_block(0, h)
    for passed in range(column):
        take(passed)
        give(passed + 1)
    passed = column
    tile_stage(1)
    for group in range(1, n_pair):
        turn(group)
        for h in range(SPLIT):
            partial_block(group, h)
    for copy in small[1:]:
        copy.wait()

    ids_m = lax.broadcasted_iota(jnp.int32, (NMOM, states), 0)
    pick_mom = (ids_m == mom_ref[...]).astype(jnp.bfloat16)
    ids_f = lax.broadcasted_iota(jnp.int32, (LANES, states), 0)
    pick_freq = (ids_f == freq_ref[...]).astype(jnp.bfloat16)

    def cells(slot):
        if slot == ACROSS:
            send_back().wait_recv()
            weight_across[...] = (
                tile_sum[...] + back_recv[...].astype(jnp.float32)
            ).astype(jnp.bfloat16)
        weight = weight_own if slot == OWN else weight_across
        folded = contract(pick_mom, greens[slot], ((1,), (0,)))
        folded = jnp.where(p == 0, folded[:, :half], folded[:, half:])
        high = folded.astype(jnp.bfloat16)
        low = (folded - high.astype(jnp.float32)).astype(jnp.bfloat16)
        joined = (contract(high, weight[...], ((1,), (0,)))
                  + contract(low, weight[...], ((1,), (0,))))
        picked = contract(pick_freq, greens[slot], ((1,), (0,)))
        value = contract(joined, picked, ((1,), (1,)), lax.Precision.HIGHEST)
        cells_ref[...] = value if slot == OWN else cells_ref[...] + value

    own_cells = NMOM * NFREQ // count

    def owner(i):
        to = lax.rem(me + i, count)
        return remote(sig_send.at[to], sig_recv.at[i - 1], s_send.at[i - 1], s_recv.at[i - 1],
                      (to // n_pair, lax.rem(to, n_pair)))

    def sigma():
        value_cells = cells_ref[...]
        rows_d = lax.broadcasted_iota(jnp.int32, (count, NMOM), 0)
        cols_m = lax.broadcasted_iota(jnp.int32, (count, NMOM), 1)
        spread = jnp.zeros((count, LANES), jnp.float32)
        if own_cells >= NFREQ:
            group = own_cells // NFREQ
            for k in range(group):
                pick = (cols_m == rows_d * group + k).astype(jnp.float32)
                value = contract(pick, value_cells, ((1,), (0,)), lax.Precision.HIGHEST)
                spread = spread + (pltpu.roll(value, NFREQ * k, 1) if k else value)
        else:
            group = NFREQ // own_cells
            for k in range(group):
                pick = (rows_d == cols_m * group + k).astype(jnp.float32)
                value = contract(pick, value_cells, ((1,), (0,)), lax.Precision.HIGHEST)
                spread = spread + (pltpu.roll(value, LANES - own_cells * k, 1) if k else value)
        factor = 1.0 / math.sqrt(5.0 * n_tiles * n_blk * states * states / (NMOM * NFREQ))
        sig_send[...] = (spread * (factor * out_scale)).reshape(count, 1, LANES)

        def send_cells(i, carry):
            owner(i).start()
            return carry

        lax.fori_loop(1, count, send_cells, 0)

    share = n_tiles // 2

    def compute_inner(slot, part):
        upper = greens[slot, own_rows, :]
        for t in range(part * share, (part + 1) * share):
            inner[slot, pl.ds(t * half, half), :] = contract(
                upper, tiles[t], ((1,), (0,))).astype(jnp.bfloat16)

    started = set()
    pending = {(0, part): 5 for part in range(2)} | {(1, part): 7 for part in range(2)}

    def compute_chi(group, slot, part, k_half=None):
        rows = own_rows if group == 0 else rest_rows
        cols = pl.ds(0, states) if k_half is None else pl.ds(k_half * wide, wide)
        first = (group, part) not in started
        started.add((group, part))
        pending[group, part] -= 1
        last = pending[group, part] == 0
        for t in range(part * share, (part + 1) * share):
            lines = pl.ds(t * half, half)
            value = contract(inner[slot, lines, cols], greens[slot, rows, cols], ((1,), (1,)))
            if not first:
                value = acc[group, lines, :] + value
            if last:
                out_ref[t, :, rows] = (value * out_scale).astype(jnp.bfloat16)
            else:
                acc[group, lines, :] = value

    def take_y(k):
        rows = chunk(p, k)
        exchange(k, p).wait_recv()
        greens[OWN, *rows] = (
            partial[*rows] + arrived[*rows].astype(jnp.float32)
        ).astype(jnp.bfloat16)
        to_across(k).start()
        to_peer(k).start()

    def take_x(k):
        to_across(k).wait_recv()
        if k < middle:
            to_along(k).start()
        else:
            @pl.when(jnp.logical_not(wrap_send))
            def _():
                to_along(k).start()

        @pl.when(forwards_across)
        def _():
            forward(ACROSS, k).start()

    def take_z(k):
        to_along(k).wait_recv()
        if k < middle:
            @pl.when(wrap_recv)
            def _():
                to_other(k).start()

        @pl.when(jnp.logical_not(forwards_across))
        def _():
            forward(RELAYED, k).start()

    waited = {"p": 0, "f": 0}

    def need(kind, k):
        if kind in waited:
            while waited[kind] <= k:
                at = waited[kind]
                (to_peer(at) if kind == "p" else forward(ACROSS, at)).wait_recv()
                waited[kind] += 1

    for task in plan(total):
        kind = task[0]
        if kind == "y":
            take_y(task[1])
        elif kind == "x":
            take_x(task[1])
            if passed < rounds - 1:
                take(passed)
                passed += 1
                give(passed)
        elif kind == "z":
            take_z(task[1])
        elif kind == "need":
            need(task[1], task[2])
        elif kind == "cells":
            cells(task[1])
        elif kind == "sigma":
            while passed < rounds - 1:
                take(passed)
                passed += 1
                give(passed)
            take(passed)
            sigma()
        elif kind == "inner":
            compute_inner(task[1], task[2])
        elif kind == "own":
            compute_chi(0, task[1], task[2])
        elif kind == "rest":
            compute_chi(1, task[1], task[3], None if task[1] < RELAYED else task[2])

    for k in range(total):
        exchange(k, 1 - p).wait_send()
        to_across(k).wait_send()
        to_peer(k).wait_send()
        forward(ACROSS, k).wait_send()
        if k < middle:
            to_along(k).wait_send()

            @pl.when(wrap_recv)
            def _():
                to_other(k).wait_send()
        else:
            @pl.when(jnp.logical_not(wrap_send))
            def _():
                to_along(k).wait_send()
    send_tiles().wait_send()
    send_back().wait_send()

    def take_cells(i, carry):
        owner(i).wait()
        return carry

    lax.fori_loop(1, count, take_cells, 0)
    summed = jnp.sum(sig_recv[...], axis=0) + sig_send[me]
    sigma_ref[...] = summed[0, :own_cells]


def solution(mesh):
    n_blk, n_pair = mesh.shape["blk"], mesh.shape["pair"]
    count = n_blk * n_pair

    def per_device(vertex, left_phase, right_phase, tiles, orders, momentum, frequency):
        height, breadth = vertex.shape[1], vertex.shape[2]
        states = right_phase.shape[2]
        n_tiles = tiles.shape[0]
        half = states // n_pair
        sizes = (n_blk, n_pair, height, breadth, states, n_tiles)
        bf16, f32 = jnp.bfloat16, jnp.float32
        dma = pltpu.SemaphoreType.DMA
        chunks = n_pair * SPLIT * (half // SIZE)
        rounds = max(n_blk // 4 - 2, 0) + 2
        chi, cells = pl.pallas_call(
            lambda *refs: body(sizes, *refs),
            out_shape=(
                pltpu.VMEM((n_tiles, half, states), bf16),
                pltpu.VMEM((NMOM * NFREQ // count,), f32),
            ),
            in_specs=[pl.BlockSpec(memory_space=pltpu.HBM)] * 7,
            out_specs=(pl.BlockSpec(memory_space=pltpu.VMEM),) * 2,
            scratch_shapes=[
                pltpu.SMEM((1,), jnp.int32),
                pltpu.VMEM((1, states), jnp.int32),
                pltpu.VMEM((1, states), jnp.int32),
                dma((3,)),
                pltpu.VMEM((height, breadth), bf16),
                pltpu.VMEM((height, states), bf16),
                pltpu.VMEM((n_pair, half, height), bf16),
                pltpu.VMEM((SPLIT, breadth, states // SPLIT), bf16),
                pltpu.VMEM((n_tiles, states, states), bf16),
                pltpu.VMEM((SPLIT, height, states // SPLIT), bf16),
                pltpu.VMEM((states, states), f32),
                pltpu.VMEM((states, states), bf16),
                pltpu.VMEM((states, states), bf16),
                pltpu.VMEM((5, states, states), bf16),
                pltpu.VMEM((5, n_tiles * half, states), bf16),
                pltpu.VMEM((2, n_tiles * half, half), f32),
                pltpu.VMEM((half, states), f32),
            ] + [pltpu.VMEM((half, states), bf16)] * 6 + [
                pltpu.VMEM((NMOM, LANES), f32),
                pltpu.VMEM((count, 1, LANES), f32),
                pltpu.VMEM((count - 1, 1, LANES), f32),
                dma((SPLIT + PIECES + 2,)),
            ] + [dma((chunks,))] * 11 + [dma((2,))] * 2 + [dma((count - 1,))] * 2 + [
                pltpu.SemaphoreType.REGULAR((rounds,))],
            compiler_params=pltpu.CompilerParams(
                collective_id=0, has_side_effects=True, vmem_limit_bytes=60 * 1024 * 1024
            ),
            name="measure_green",
        )(
            orders,
            momentum.reshape(1, states),
            frequency.reshape(1, states),
            vertex,
            left_phase,
            right_phase,
            tiles,
        )
        return chi, cells

    in_specs = (
        P("blk", "pair", None),
        P("blk", "pair", None),
        P("blk", None, None),
        P("blk", None, None),
        P("blk"),
        P(),
        P(),
    )
    out_specs = (P("blk", "pair", None), P(("blk", "pair")))
    return jax.shard_map(
        per_device, mesh=mesh, in_specs=in_specs, out_specs=out_specs, check_vma=False
    )
```

```python
import math

import jax
import jax.numpy as jnp
from jax import lax
from jax.experimental import pallas as pl
from jax.experimental.pallas import tpu as pltpu
from jax.sharding import PartitionSpec as P

NMOM = 64
NFREQ = 32
LANES = 128
SIZE = 128
SPLIT = 2
PIECES = 8
MESH = pl.DeviceIdType.MESH
OWN, PEER, ACROSS, RELAYED, FORWARDED = range(5)

FIRST, HOP, NEAR, LATE, LAST, STEP = 8.2, 1.9, 1.0, 3.0, 4.0, 1.41
INNER, CHI = 0.2, 0.11


def contract(a, b, dims, precision=None):
    return lax.dot_general(
        a, b, (dims, ((), ())), preferred_element_type=jnp.float32, precision=precision
    )


def plan(count, parts):
    step = STEP * 8 / count
    half = count // 2
    quarter = count // 4
    arrive = {}
    for k in range(count):
        y = FIRST + step * (k + 1)
        arrive["y", k] = y
        arrive["x", k] = y + step + HOP
        arrive["z", k] = y + 2 * (step + HOP) + (LATE if k < half else max(LAST - LATE, 0.0))
        arrive["p", k] = y + NEAR
    for k in range(half, count):
        arrive["z", k] = max(arrive["z", k], arrive["z", k - half] + step + HOP)
    for k in range(count):
        arrive["f", k] = arrive["z", k] + NEAR
    source = {OWN: "y", PEER: "p", ACROSS: "x", RELAYED: "z", FORWARDED: "f"}
    jobs = []
    for slot in range(5):
        s = source[slot]
        for part in range(parts):
            jobs.append((arrive[s, half - 1], INNER, ("inner", slot, part), [(s, half - 1)], []))
        for part in range(parts):
            jobs.append((arrive[s, half - 1], CHI, ("own", slot, part), [(s, half - 1)],
                         [("inner", slot, part)]))
        for h in range(2):
            k = half + quarter * (h + 1) - 1
            if slot < RELAYED and h == 0:
                continue
            for part in range(parts):
                length = CHI if slot < RELAYED else CHI / 2
                jobs.append((arrive[s, k], length, ("rest", slot, h, part), [(s, k)],
                             [("inner", slot, part)]))
    jobs.append((arrive["y", count - 1], 0.3, ("cells", OWN), [("y", count - 1)], []))
    jobs.append((arrive["x", count - 1], 0.3, ("cells", ACROSS), [("x", count - 1)],
                 [("cells", OWN)]))
    jobs.append((arrive["x", count - 1], 0.3, ("sigma",), [("x", count - 1)], [("cells", ACROSS)]))
    urgent = {"cells": 1, "sigma": 1, "inner": 2, "own": 3, "rest": 3}
    waits = sorted((t, key) for key, t in arrive.items() if key[0] in "yxz")
    order, done, now = [], set(), 0.0
    taken = set()
    while waits or jobs:
        if waits and waits[0][0] <= now + 0.05:
            t, key = waits.pop(0)
            now = max(now, t)
            order.append(key)
            taken.add(key)
            continue
        ready = [j for j in jobs if j[0] <= now and all(d in done for d in j[4])
                 and all(w in taken or w[0] in "pf" for w in j[3])]
        if ready:
            job = min(ready, key=lambda j: (urgent[j[2][0]], j[0]))
            jobs.remove(job)
            for w in job[3]:
                order.append(("need",) + w)
            order.append(job[2])
            done.add(job[2])
            now += job[1]
            continue
        times = [j[0] for j in jobs if j[0] > now] + ([waits[0][0]] if waits else [])
        now = min(times)
    return order


def body(sizes, order_hbm, mom_hbm, freq_hbm, vertex_hbm, left_hbm, right_hbm, tiles_hbm,
         out_ref, sigma_ref,
         order_ref, mom_ref, freq_ref, small_sem, vertex, left, turned, right, tiles, carried, partial, sending, arrived, greens, inner, acc,
         tile_sum, tile_send, tile_recv, back_send, back_recv, weight_own, weight_across,
         cells_ref, sig_send, sig_recv, load_sem, y_send, y_recv, x_send, x_recv, z_send, z_recv,
         p_send, p_recv, f_send, f_recv, w_send, t_send, t_recv, s_send, s_recv, token):
    n_blk, n_pair, height, breadth, states, n_tiles = sizes
    count = n_blk * n_pair
    half = states // n_pair
    b = lax.axis_index("blk")
    p = lax.axis_index("pair")
    me = b * n_pair + p
    chip = b // 2
    core = lax.rem(b, 2)
    odd = lax.rem(chip, 2)
    step = 1 - 2 * odd
    across = (lax.rem(b + 2 * step + n_blk, n_blk), p)
    along = (lax.rem(b + 4 * step + n_blk, n_blk), p)
    back = (lax.rem(b - 4 * step + n_blk, n_blk), p)
    peer = (b + 1 - 2 * core, p)
    other = (b, 1 - p)
    forwards_across = lax.rem(odd + core, 2) == 0
    low_end = b < 4
    high_end = b >= n_blk - 4
    even = odd == 0
    wrap_send = jnp.logical_or(jnp.logical_and(even, high_end),
                               jnp.logical_and(jnp.logical_not(even), low_end))
    wrap_recv = jnp.logical_or(jnp.logical_and(even, low_end),
                               jnp.logical_and(jnp.logical_not(even), high_end))

    barrier = pltpu.get_barrier_semaphore()

    def tell(semaphore, devices):
        for device in devices:
            pl.semaphore_signal(semaphore, inc=1, device_id=device, device_id_type=MESH)

    def tell_column(semaphore):
        @pl.when(jnp.logical_not(wrap_send))
        def _():
            tell(semaphore, (along,))

        @pl.when(jnp.logical_not(wrap_recv))
        def _():
            tell(semaphore, (back,))

    beside = 2 - wrap_send.astype(jnp.int32) - wrap_recv.astype(jnp.int32)
    tell(barrier, (other, across, peer))
    tell_column(barrier)

    pieces = PIECES
    block = height // pieces
    wide = states // SPLIT

    def load_right(h):
        cols = pl.ds(h * wide, wide)
        return pltpu.make_async_copy(right_hbm.at[0, :, cols], right.at[h], load_sem.at[h])

    small = [
        pltpu.make_async_copy(order_hbm, order_ref, small_sem.at[0]),
        pltpu.make_async_copy(mom_hbm, mom_ref, small_sem.at[1]),
        pltpu.make_async_copy(freq_hbm, freq_ref, small_sem.at[2]),
    ]
    load_left = pltpu.make_async_copy(left_hbm.at[0], left, load_sem.at[SPLIT + pieces])
    load_tiles = pltpu.make_async_copy(tiles_hbm, tiles, load_sem.at[SPLIT + 1 + pieces])
    load_vertex = []
    for i in range(pieces):
        rows = pl.ds(i * block, block)
        load_vertex.append(
            pltpu.make_async_copy(vertex_hbm.at[0, rows], vertex.at[rows], load_sem.at[SPLIT + i]))
    queue = list(load_vertex) + [load_right(h) for h in range(1, SPLIT)] + [load_tiles] + small[1:]

    def pump(number):
        for copy in queue[:number]:
            copy.start()
        del queue[:number]

    small[0].start()
    load_left.start()
    load_right(0).start()
    pump(3)

    scale = 1.0 / math.sqrt(breadth)
    per = half // SIZE
    total = n_pair * SPLIT * per
    middle = total // 2

    def chunk(which, k):
        group, h, i = k // (SPLIT * per), k // per % SPLIT, k % per
        start = lax.rem(which + group, n_pair) * half + i * SIZE
        return pl.ds(pl.multiple_of(start, SIZE), SIZE), pl.ds(h * wide, wide)

    def remote(src, dst, send, recv, device):
        return pltpu.make_async_remote_copy(src_ref=src, dst_ref=dst, send_sem=send, recv_sem=recv,
                                            device_id=device, device_id_type=MESH)

    def exchange(k, which):
        rows = chunk(which, k)
        return remote(sending.at[*rows], arrived.at[*rows], y_send.at[0], y_recv.at[k], other)

    def hop(source, target, k, send, recv, device):
        rows = chunk(p, k)
        return remote(greens.at[source, *rows], greens.at[target, *rows], send, recv, device)

    def to_across(k):
        return hop(OWN, ACROSS, k, x_send.at[0], x_recv.at[k], across)

    def to_peer(k):
        return hop(OWN, PEER, k, p_send.at[0], p_recv.at[k], peer)

    def to_along(k):
        return hop(ACROSS, RELAYED, k, z_send.at[k // middle], z_recv.at[k], along)

    def to_other(k):
        return hop(RELAYED, RELAYED, k, w_send.at[0], z_recv.at[k + middle], other)

    def forward(source, k):
        return hop(source, FORWARDED, k, f_send.at[0], f_recv.at[k], peer)

    def send_tiles():
        return remote(tile_send, tile_recv, t_send.at[0], t_recv.at[0], peer)

    def send_back():
        return remote(back_send, back_recv, t_send.at[1], t_recv.at[1], back)

    column = max(n_blk // 4 - 2, 0)
    rounds = column + 2

    def give(r):
        if r < column:
            tell_column(token.at[r])
        else:
            tell(token.at[r], (other, across, peer))

    def take(r):
        pl.semaphore_wait(token.at[r], beside if r < column else 3)

    def mask_right(h):
        def part(i, carry):
            rows = pl.ds(pl.multiple_of(i * 256, 256), 256)
            ids = i * 256 + lax.broadcasted_iota(jnp.int32, (256, wide), 0)
            right[h, rows, :] = jnp.where(ids < order, right[h, rows, :],
                                          jnp.zeros((), jnp.bfloat16))
            return carry

        lax.fori_loop(0, breadth // 256, part, 0)

    def carry_half(h):
        for i in range(pieces):
            rows = pl.ds(i * block, block)
            if h == 0:
                load_vertex[i].wait()
                pump(1)
            product = contract(vertex[rows, :], right[h], ((1,), (0,)))
            ids = p * height + i * block + lax.broadcasted_iota(jnp.int32, (block, wide), 0)
            carried[h, rows, :] = jnp.where(ids < order, product, 0.0).astype(jnp.bfloat16)
            if h == 0 and i % 2 == 1:
                first_block(i // 2)

    def first_block(i):
        rows = pl.ds(pl.multiple_of((1 - p) * half, half), half)
        depth = pl.ds(2 * i * block, 2 * block)
        product = contract(turned[0, :, depth], carried[0, depth, :], ((1,), (0,))) * scale
        if i > 0:
            product = partial[rows, pl.ds(0, wide)] + product
        partial[rows, pl.ds(0, wide)] = product
        if i == pieces // 2 - 1:
            sending[rows, pl.ds(0, wide)] = product.astype(jnp.bfloat16)

    def send_block(group, h):
        for i in range(per):
            exchange((group * SPLIT + h) * per + i, 1 - p).start()

    def partial_block(group, h):
        which = lax.rem(1 - p + group, n_pair)
        rows = pl.ds(pl.multiple_of(which * half, half), half)
        cols = pl.ds(h * wide, wide)
        product = contract(turned[group], carried[h], ((1,), (0,))) * scale
        partial[rows, cols] = product
        sending[rows, cols] = product.astype(jnp.bfloat16)
        send_block(group, h)

    def turn(group):
        which = lax.rem(1 - p + group, n_pair)
        cols = pl.ds(pl.multiple_of(which * half, half), half)
        turned[group] = left[:, cols].T

    own_rows = pl.ds(pl.multiple_of(p * half, half), half)
    rest_rows = pl.ds(pl.multiple_of((1 - p) * half, half), half)
    out_scale = 1.0 / math.sqrt(states)
    pair_share = forwards_across.astype(jnp.float32)

    def tile_stage(stage):
        if stage == 0:
            value = tiles[0, own_rows, :].astype(jnp.float32)
            for t in range(1, n_tiles):
                value = value + tiles[t, own_rows, :].astype(jnp.float32)
            tile_sum[...] = value
            tile_send[...] = value.astype(jnp.bfloat16)
            send_tiles().start()
        else:
            send_tiles().wait_recv()
            mine = tile_sum[...]
            theirs = tile_recv[...].astype(jnp.float32)
            back_send[...] = (mine + (1.0 - pair_share) * theirs).astype(jnp.bfloat16)
            send_back().start()
            weight_own[...] = (mine + theirs).astype(jnp.bfloat16)
            tile_sum[...] = mine + pair_share * theirs

    small[0].wait()
    order = order_ref[0]
    load_left.wait()
    pump(2)
    turn(0)
    load_right(0).wait()
    pump(2)
    mask_right(0)
    carry_half(0)
    pump(len(queue))
    pl.semaphore_wait(barrier, 3 + beside)
    send_block(0, 0)
    passed = 0
    give(passed)
    load_tiles.wait()
    tile_stage(0)
    for h in range(1, SPLIT):
        load_right(h).wait()
        mask_right(h)
        carry_half(h)
        partial_block(0, h)
    for passed in range(column):
        take(passed)
        give(passed + 1)
    passed = column
    tile_stage(1)
    for group in range(1, n_pair):
        turn(group)
        for h in range(SPLIT):
            partial_block(group, h)
    for copy in small[1:]:
        copy.wait()

    own_cells = NMOM * NFREQ // count
    folds = max(own_cells // NFREQ, 1)
    ids_m = lax.broadcasted_iota(jnp.int32, (NMOM, states), 0)
    ids_m = lax.rem(ids_m, NMOM // folds) * folds + ids_m // (NMOM // folds)
    pick_mom = (ids_m == mom_ref[...]).astype(jnp.bfloat16)
    ids_f = lax.broadcasted_iota(jnp.int32, (LANES, states), 0)
    pick_freq = (ids_f == freq_ref[...]).astype(jnp.bfloat16)

    def split(value):
        high = value.astype(jnp.bfloat16)
        low = (value - high.astype(jnp.float32)).astype(jnp.bfloat16)
        return jnp.concatenate([high, low], axis=0)

    def cells(slot):
        if slot == ACROSS:
            send_back().wait_recv()
            weight_across[...] = (
                tile_sum[...] + back_recv[...].astype(jnp.float32)
            ).astype(jnp.bfloat16)
        weight = weight_own if slot == OWN else weight_across
        folded = contract(pick_mom, greens[slot], ((1,), (0,)))
        folded = jnp.where(p == 0, folded[:, :half], folded[:, half:])
        joined = contract(split(folded), weight[...], ((1,), (0,)))
        joined = split(joined[:NMOM] + joined[NMOM:])
        picked = split(contract(pick_freq, greens[slot], ((1,), (0,))))
        value = contract(joined, picked[:LANES], ((1,), (1,)))
        value = (value[:NMOM] + value[NMOM:]
                 + contract(joined[:NMOM], picked[LANES:], ((1,), (1,))))
        cells_ref[...] = value if slot == OWN else cells_ref[...] + value

    def owner(i):
        to = lax.rem(me + i, count)
        return remote(sig_send.at[to], sig_recv.at[i - 1], s_send.at[0], s_recv.at[0],
                      (to // n_pair, lax.rem(to, n_pair)))

    def sigma():
        value_cells = cells_ref[...]
        rows_d = lax.broadcasted_iota(jnp.int32, (count, NMOM), 0)
        cols_m = lax.broadcasted_iota(jnp.int32, (count, NMOM), 1)
        spread = jnp.zeros((count, LANES), jnp.float32)
        if own_cells >= NFREQ:
            for k in range(folds):
                value = value_cells[k * count:(k + 1) * count, :]
                spread = spread + (pltpu.roll(value, NFREQ * k, 1) if k else value)
        else:
            group = NFREQ // own_cells
            for k in range(group):
                pick = (rows_d == cols_m * group + k).astype(jnp.float32)
                value = contract(pick, value_cells, ((1,), (0,)), lax.Precision.HIGHEST)
                spread = spread + (pltpu.roll(value, LANES - own_cells * k, 1) if k else value)
        factor = 1.0 / math.sqrt(5.0 * n_tiles * n_blk * states * states / (NMOM * NFREQ))
        sig_send[...] = (spread * (factor * out_scale)).reshape(count, 1, LANES)

        if count <= 32:
            for i in range(1, count):
                owner(i).start()
        else:
            def send_cells(i, carry):
                owner(i).start()
                return carry

            lax.fori_loop(1, count, send_cells, 0)

    def compute_inner(slot, part):
        upper = greens[slot, own_rows, :]
        for t in (part,):
            inner[slot, pl.ds(t * half, half), :] = contract(
                upper, tiles[t], ((1,), (0,))).astype(jnp.bfloat16)

    started = set()
    pending = {(0, part): 5 for part in range(n_tiles)} | {(1, part): 7 for part in range(n_tiles)}

    def compute_chi(group, slot, part, k_half=None):
        rows = own_rows if group == 0 else rest_rows
        cols = pl.ds(0, states) if k_half is None else pl.ds(k_half * wide, wide)
        first = (group, part) not in started
        started.add((group, part))
        pending[group, part] -= 1
        last = pending[group, part] == 0
        for t in (part,):
            lines = pl.ds(t * half, half)
            value = contract(inner[slot, lines, cols], greens[slot, rows, cols], ((1,), (1,)))
            if not first:
                value = acc[group, lines, :] + value
            if last:
                out_ref[t, :, rows] = (value * out_scale).astype(jnp.bfloat16)
            else:
                acc[group, lines, :] = value

    def take_y(k):
        rows = chunk(p, k)
        exchange(k, p).wait_recv()
        greens[OWN, *rows] = (
            partial[*rows] + arrived[*rows].astype(jnp.float32)
        ).astype(jnp.bfloat16)
        to_across(k).start()
        to_peer(k).start()

    def take_x(k):
        to_across(k).wait_recv()
        if k < middle:
            to_along(k).start()
        else:
            @pl.when(jnp.logical_not(wrap_send))
            def _():
                to_along(k).start()

        @pl.when(forwards_across)
        def _():
            forward(ACROSS, k).start()

    def take_z(k):
        to_along(k).wait_recv()
        if k < middle:
            @pl.when(wrap_recv)
            def _():
                to_other(k).start()

        @pl.when(jnp.logical_not(forwards_across))
        def _():
            forward(RELAYED, k).start()

    waited = {"p": 0, "f": 0}

    def need(kind, k):
        if kind in waited:
            while waited[kind] <= k:
                at = waited[kind]
                (to_peer(at) if kind == "p" else forward(ACROSS, at)).wait_recv()
                waited[kind] += 1

    for task in plan(total, n_tiles):
        kind = task[0]
        if kind == "y":
            take_y(task[1])
        elif kind == "x":
            take_x(task[1])
            if passed < rounds - 1:
                take(passed)
                passed += 1
                give(passed)
        elif kind == "z":
            take_z(task[1])
        elif kind == "need":
            need(task[1], task[2])
        elif kind == "cells":
            cells(task[1])
        elif kind == "sigma":
            while passed < rounds - 1:
                take(passed)
                passed += 1
                give(passed)
            take(passed)
            sigma()
        elif kind == "inner":
            compute_inner(task[1], task[2])
        elif kind == "own":
            compute_chi(0, task[1], task[2])
        elif kind == "rest":
            compute_chi(1, task[1], task[3], None if task[1] < RELAYED else task[2])

    remote(sending, arrived, y_send.at[0], y_recv.at[0], other).wait_send()
    remote(greens.at[OWN], greens.at[ACROSS], x_send.at[0], x_recv.at[0], across).wait_send()
    remote(greens.at[OWN], greens.at[PEER], p_send.at[0], p_recv.at[0], peer).wait_send()
    remote(greens.at[ACROSS], greens.at[FORWARDED], f_send.at[0], f_recv.at[0], peer).wait_send()
    upper = pl.ds(0, half)
    remote(greens.at[ACROSS, upper], greens.at[RELAYED, upper], z_send.at[0], z_recv.at[0],
           along).wait_send()

    @pl.when(jnp.logical_not(wrap_send))
    def _():
        remote(greens.at[ACROSS, upper], greens.at[RELAYED, upper], z_send.at[1], z_recv.at[0],
               along).wait_send()

    @pl.when(wrap_recv)
    def _():
        remote(greens.at[RELAYED, upper], greens.at[RELAYED, upper], w_send.at[0], z_recv.at[0],
               other).wait_send()

    send_tiles().wait_send()
    send_back().wait_send()

    cell_block = remote(sig_send.at[pl.ds(0, count - 1)], sig_recv, s_send.at[0], s_recv.at[0], peer)
    cell_block.wait_send()
    cell_block.wait_recv()
    summed = jnp.sum(sig_recv[...], axis=0) + sig_send[me]
    sigma_ref[...] = summed[0, :own_cells]


def solution(mesh):
    n_blk, n_pair = mesh.shape["blk"], mesh.shape["pair"]
    count = n_blk * n_pair

    def per_device(vertex, left_phase, right_phase, tiles, orders, momentum, frequency):
        height, breadth = vertex.shape[1], vertex.shape[2]
        states = right_phase.shape[2]
        n_tiles = tiles.shape[0]
        half = states // n_pair
        sizes = (n_blk, n_pair, height, breadth, states, n_tiles)
        bf16, f32 = jnp.bfloat16, jnp.float32
        dma = pltpu.SemaphoreType.DMA
        chunks = n_pair * SPLIT * (half // SIZE)
        rounds = max(n_blk // 4 - 2, 0) + 2
        chi, cells = pl.pallas_call(
            lambda *refs: body(sizes, *refs),
            out_shape=(
                pltpu.VMEM((n_tiles, half, states), bf16),
                pltpu.VMEM((NMOM * NFREQ // count,), f32),
            ),
            in_specs=[pl.BlockSpec(memory_space=pltpu.HBM)] * 7,
            out_specs=(pl.BlockSpec(memory_space=pltpu.VMEM),) * 2,
            scratch_shapes=[
                pltpu.SMEM((1,), jnp.int32),
                pltpu.VMEM((1, states), jnp.int32),
                pltpu.VMEM((1, states), jnp.int32),
                dma((3,)),
                pltpu.VMEM((height, breadth), bf16),
                pltpu.VMEM((height, states), bf16),
                pltpu.VMEM((n_pair, half, height), bf16),
                pltpu.VMEM((SPLIT, breadth, states // SPLIT), bf16),
                pltpu.VMEM((n_tiles, states, states), bf16),
                pltpu.VMEM((SPLIT, height, states // SPLIT), bf16),
                pltpu.VMEM((states, states), f32),
                pltpu.VMEM((states, states), bf16),
                pltpu.VMEM((states, states), bf16),
                pltpu.VMEM((5, states, states), bf16),
                pltpu.VMEM((5, n_tiles * half, states), bf16),
                pltpu.VMEM((2, n_tiles * half, half), f32),
                pltpu.VMEM((half, states), f32),
            ] + [pltpu.VMEM((half, states), bf16)] * 6 + [
                pltpu.VMEM((NMOM, LANES), f32),
                pltpu.VMEM((count, 1, LANES), f32),
                pltpu.VMEM((count - 1, 1, LANES), f32),
                dma((SPLIT + PIECES + 2,)),
            ] + [dma((1,)), dma((chunks,))] * 2 + [dma((2,)), dma((chunks,))] + [dma((1,)), dma((chunks,))] * 2 + [
                dma((1,))] + [dma((2,))] * 2 + [dma((1,))] * 2 + [
                pltpu.SemaphoreType.REGULAR((rounds,))],
            compiler_params=pltpu.CompilerParams(
                collective_id=0, has_side_effects=True, vmem_limit_bytes=60 * 1024 * 1024
            ),
            name="measure_green",
        )(
            orders,
            momentum.reshape(1, states),
            frequency.reshape(1, states),
            vertex,
            left_phase,
            right_phase,
            tiles,
        )
        return chi, cells

    in_specs = (
        P("blk", "pair", None),
        P("blk", "pair", None),
        P("blk", None, None),
        P("blk", None, None),
        P("blk"),
        P(),
        P(),
    )
    out_specs = (P("blk", "pair", None), P(("blk", "pair")))
    return jax.shard_map(
        per_device, mesh=mesh, in_specs=in_specs, out_specs=out_specs, check_vma=False
    )
```

```python
import math

import jax
import jax.numpy as jnp
from jax import lax
from jax.experimental import pallas as pl
from jax.experimental.pallas import tpu as pltpu
from jax.sharding import PartitionSpec as P

NMOM = 64
NFREQ = 32
LANES = 128
SIZE = 128
SPLIT = 2
PIECES = 8
MESH = pl.DeviceIdType.MESH
OWN, PEER, ACROSS, RELAYED, FORWARDED = range(5)

FIRST, HOP, NEAR, LATE, LAST, STEP = 8.2, 1.9, 1.0, 3.0, 4.0, 1.41
INNER, CHI = 0.2, 0.11


def contract(a, b, dims, precision=None):
    return lax.dot_general(
        a, b, (dims, ((), ())), preferred_element_type=jnp.float32, precision=precision
    )


def plan(count, parts):
    step = STEP * 8 / count
    half = count // 2
    quarter = count // 4
    arrive = {}
    for k in range(count):
        y = FIRST + step * (k + 1)
        arrive["y", k] = y
        arrive["x", k] = y + step + HOP
        arrive["z", k] = y + 2 * (step + HOP) + (LATE if k < half else max(LAST - LATE, 0.0))
        arrive["p", k] = y + NEAR
    for k in range(half, count):
        arrive["z", k] = max(arrive["z", k], arrive["z", k - half] + step + HOP)
    for k in range(count):
        arrive["f", k] = arrive["z", k] + NEAR
    source = {OWN: "y", PEER: "p", ACROSS: "x", RELAYED: "z", FORWARDED: "f"}
    jobs = []
    for slot in range(5):
        s = source[slot]
        for part in range(parts):
            jobs.append((arrive[s, half - 1], INNER, ("inner", slot, part), [(s, half - 1)], []))
        for part in range(parts):
            jobs.append((arrive[s, half - 1], CHI, ("own", slot, part), [(s, half - 1)],
                         [("inner", slot, part)]))
        for h in range(2):
            k = half + quarter * (h + 1) - 1
            if slot < RELAYED and h == 0:
                continue
            for part in range(parts):
                length = CHI if slot < RELAYED else CHI / 2
                jobs.append((arrive[s, k], length, ("rest", slot, h, part), [(s, k)],
                             [("inner", slot, part)]))
    jobs.append((arrive["y", count - 1], 0.3, ("cells", OWN), [("y", count - 1)], []))
    jobs.append((arrive["x", count - 1], 0.3, ("cells", ACROSS), [("x", count - 1)],
                 [("cells", OWN)]))
    jobs.append((arrive["x", count - 1], 0.3, ("sigma",), [("x", count - 1)], [("cells", ACROSS)]))
    urgent = {"cells": 1, "sigma": 1, "inner": 2, "own": 3, "rest": 3}
    waits = sorted((t, key) for key, t in arrive.items() if key[0] in "yxz")
    order, done, now = [], set(), 0.0
    taken = set()
    while waits or jobs:
        if waits and waits[0][0] <= now + 0.05:
            t, key = waits.pop(0)
            now = max(now, t)
            order.append(key)
            taken.add(key)
            continue
        ready = [j for j in jobs if j[0] <= now and all(d in done for d in j[4])
                 and all(w in taken or w[0] in "pf" for w in j[3])]
        if ready:
            job = min(ready, key=lambda j: (urgent[j[2][0]], j[0]))
            jobs.remove(job)
            for w in job[3]:
                order.append(("need",) + w)
            order.append(job[2])
            done.add(job[2])
            now += job[1]
            continue
        times = [j[0] for j in jobs if j[0] > now] + ([waits[0][0]] if waits else [])
        now = min(times)
    return order


def body(sizes, order_hbm, mom_hbm, freq_hbm, vertex_hbm, left_hbm, right_hbm, tiles_hbm,
         out_ref, sigma_ref,
         order_ref, mom_ref, freq_ref, small_sem, vertex, left, turned, right, tiles, carried, partial, sending, arrived, greens, inner, acc,
         tile_sum, tile_send, tile_recv, back_send, back_recv, weight_own, weight_across,
         cells_ref, sig_send, sig_recv, load_sem, y_send, y_recv, x_send, x_recv, z_send, z_recv,
         p_send, p_recv, f_send, f_recv, w_send, t_send, t_recv, s_send, s_recv, token):
    n_blk, n_pair, height, breadth, states, n_tiles = sizes
    count = n_blk * n_pair
    half = states // n_pair
    b = lax.axis_index("blk")
    p = lax.axis_index("pair")
    me = b * n_pair + p
    chip = b // 2
    core = lax.rem(b, 2)
    odd = lax.rem(chip, 2)
    step = 1 - 2 * odd
    across = (lax.rem(b + 2 * step + n_blk, n_blk), p)
    along = (lax.rem(b + 4 * step + n_blk, n_blk), p)
    back = (lax.rem(b - 4 * step + n_blk, n_blk), p)
    peer = (b + 1 - 2 * core, p)
    other = (b, 1 - p)
    forwards_across = lax.rem(odd + core, 2) == 0
    low_end = b < 4
    high_end = b >= n_blk - 4
    even = odd == 0
    wrap_send = jnp.logical_or(jnp.logical_and(even, high_end),
                               jnp.logical_and(jnp.logical_not(even), low_end))
    wrap_recv = jnp.logical_or(jnp.logical_and(even, low_end),
                               jnp.logical_and(jnp.logical_not(even), high_end))

    barrier = pltpu.get_barrier_semaphore()

    def tell(semaphore, devices):
        for device in devices:
            pl.semaphore_signal(semaphore, inc=1, device_id=device, device_id_type=MESH)

    def tell_column(semaphore):
        tell(semaphore, (along, back))

    beside = 2
    tell(barrier, (other, across, peer))
    tell_column(barrier)

    pieces = PIECES
    block = height // pieces
    wide = states // SPLIT

    def load_right(h):
        cols = pl.ds(h * wide, wide)
        return pltpu.make_async_copy(right_hbm.at[0, :, cols], right.at[h], load_sem.at[h])

    small = [
        pltpu.make_async_copy(order_hbm, order_ref, small_sem.at[0]),
        pltpu.make_async_copy(mom_hbm, mom_ref, small_sem.at[1]),
        pltpu.make_async_copy(freq_hbm, freq_ref, small_sem.at[2]),
    ]
    load_left = pltpu.make_async_copy(left_hbm.at[0], left, load_sem.at[SPLIT + pieces])
    load_vertex = []
    for i in range(pieces):
        rows = pl.ds(i * block, block)
        load_vertex.append(
            pltpu.make_async_copy(vertex_hbm.at[0, rows], vertex.at[rows], load_sem.at[SPLIT + i]))
    own_rows = pl.ds(pl.multiple_of(p * half, half), half)
    rest_rows = pl.ds(pl.multiple_of((1 - p) * half, half), half)
    load_tiles = [
        pltpu.make_async_copy(tiles_hbm.at[:, rows], tiles.at[:, rows], load_sem.at[at])
        for rows, at in ((own_rows, SPLIT + 1 + pieces), (rest_rows, SPLIT + 2 + pieces))
    ]
    queue = list(load_vertex) + [load_right(h) for h in range(1, SPLIT)] + load_tiles[1:] + small[1:]

    def pump(number):
        for copy in queue[:number]:
            copy.start()
        del queue[:number]

    small[0].start()
    load_left.start()
    load_right(0).start()
    load_tiles[0].start()
    pump(3)

    scale = 1.0 / math.sqrt(breadth)
    per = half // SIZE
    total = n_pair * SPLIT * per
    middle = total // 2

    def chunk(which, k):
        group, h, i = k // (SPLIT * per), k // per % SPLIT, k % per
        start = lax.rem(which + group, n_pair) * half + i * SIZE
        return pl.ds(pl.multiple_of(start, SIZE), SIZE), pl.ds(h * wide, wide)

    def remote(src, dst, send, recv, device):
        return pltpu.make_async_remote_copy(src_ref=src, dst_ref=dst, send_sem=send, recv_sem=recv,
                                            device_id=device, device_id_type=MESH)

    def exchange(k, which):
        rows = chunk(which, k)
        return remote(sending.at[*rows], arrived.at[*rows], y_send.at[0], y_recv.at[k], other)

    def hop(source, target, k, send, recv, device):
        rows = chunk(p, k)
        return remote(greens.at[source, *rows], greens.at[target, *rows], send, recv, device)

    def to_across(k):
        return hop(OWN, ACROSS, k, x_send.at[0], x_recv.at[k], across)

    def to_peer(k):
        return hop(OWN, PEER, k, p_send.at[0], p_recv.at[k], peer)

    def to_along(k):
        return hop(ACROSS, RELAYED, k, z_send.at[k // middle], z_recv.at[k], along)

    def to_other(k):
        return hop(RELAYED, RELAYED, k, w_send.at[0], z_recv.at[k + middle], other)

    def forward(source, k):
        return hop(source, FORWARDED, k, f_send.at[0], f_recv.at[k], peer)

    def send_tiles():
        return remote(tile_send, tile_recv, t_send.at[0], t_recv.at[0], peer)

    def send_back():
        return remote(back_send, back_recv, t_send.at[1], t_recv.at[1], back)

    column = max(n_blk // 8 - 1, 0)
    rounds = column + 2

    def give(r):
        if r < column:
            tell_column(token.at[r])
        else:
            tell(token.at[r], (other, across, peer))

    def take(r):
        pl.semaphore_wait(token.at[r], beside if r < column else 3)

    def mask_right(h):
        def part(i, carry):
            rows = pl.ds(pl.multiple_of(i * 256, 256), 256)
            ids = i * 256 + lax.broadcasted_iota(jnp.int32, (256, wide), 0)
            right[h, rows, :] = jnp.where(ids < order, right[h, rows, :],
                                          jnp.zeros((), jnp.bfloat16))
            return carry

        lax.fori_loop(0, breadth // 256, part, 0)

    def carry_half(h):
        for i in range(pieces):
            rows = pl.ds(i * block, block)
            if h == 0:
                load_vertex[i].wait()
                pump(1)
            product = contract(vertex[rows, :], right[h], ((1,), (0,)))
            ids = p * height + i * block + lax.broadcasted_iota(jnp.int32, (block, wide), 0)
            carried[h, rows, :] = jnp.where(ids < order, product, 0.0).astype(jnp.bfloat16)
            if h == 0 and i % 2 == 1:
                first_block(i // 2)

    def first_block(i):
        rows = pl.ds(pl.multiple_of((1 - p) * half, half), half)
        depth = pl.ds(2 * i * block, 2 * block)
        product = contract(turned[0, :, depth], carried[0, depth, :], ((1,), (0,))) * scale
        if i > 0:
            product = partial[rows, pl.ds(0, wide)] + product
        partial[rows, pl.ds(0, wide)] = product
        if i == pieces // 2 - 1:
            sending[rows, pl.ds(0, wide)] = product.astype(jnp.bfloat16)

    def send_block(group, h):
        for i in range(per):
            exchange((group * SPLIT + h) * per + i, 1 - p).start()

    def partial_block(group, h):
        which = lax.rem(1 - p + group, n_pair)
        rows = pl.ds(pl.multiple_of(which * half, half), half)
        cols = pl.ds(h * wide, wide)
        product = contract(turned[group], carried[h], ((1,), (0,))) * scale
        partial[rows, cols] = product
        sending[rows, cols] = product.astype(jnp.bfloat16)
        send_block(group, h)

    def turn(group):
        which = lax.rem(1 - p + group, n_pair)
        cols = pl.ds(pl.multiple_of(which * half, half), half)
        turned[group] = left[:, cols].T

    out_scale = 1.0 / math.sqrt(states)
    pair_share = forwards_across.astype(jnp.float32)

    def tile_stage(stage):
        if stage == 0:
            value = tiles[0, own_rows, :].astype(jnp.float32)
            for t in range(1, n_tiles):
                value = value + tiles[t, own_rows, :].astype(jnp.float32)
            tile_sum[...] = value
            tile_send[...] = value.astype(jnp.bfloat16)
        else:
            send_tiles().wait_recv()
            mine = tile_sum[...]
            theirs = tile_recv[...].astype(jnp.float32)
            back_send[...] = (mine + (1.0 - pair_share) * theirs).astype(jnp.bfloat16)
            send_back().start()
            weight_own[...] = (mine + theirs).astype(jnp.bfloat16)
            tile_sum[...] = mine + pair_share * theirs

    small[0].wait()
    order = order_ref[0]
    load_left.wait()
    pump(2)
    turn(0)
    load_right(0).wait()
    pump(2)
    mask_right(0)
    load_tiles[0].wait()
    tile_stage(0)
    carry_half(0)
    pump(len(queue))
    pl.semaphore_wait(barrier, 3 + beside)
    send_block(0, 0)
    send_tiles().start()
    passed = 0
    give(passed)
    load_tiles[1].wait()
    for h in range(1, SPLIT):
        load_right(h).wait()
        mask_right(h)
        carry_half(h)
        partial_block(0, h)
    tile_stage(1)
    for group in range(1, n_pair):
        turn(group)
        for h in range(SPLIT):
            partial_block(group, h)
    for copy in small[1:]:
        copy.wait()

    own_cells = NMOM * NFREQ // count
    folds = max(own_cells // NFREQ, 1)
    ids_m = lax.broadcasted_iota(jnp.int32, (NMOM, states), 0)
    ids_m = lax.rem(ids_m, NMOM // folds) * folds + ids_m // (NMOM // folds)
    pick_mom = (ids_m == mom_ref[...]).astype(jnp.bfloat16)
    ids_f = lax.broadcasted_iota(jnp.int32, (LANES, states), 0)
    pick_freq = (ids_f == freq_ref[...]).astype(jnp.bfloat16)

    def split(value):
        high = value.astype(jnp.bfloat16)
        low = (value - high.astype(jnp.float32)).astype(jnp.bfloat16)
        return jnp.concatenate([high, low], axis=0)

    def cells(slot):
        if slot == ACROSS:
            send_back().wait_recv()
            weight_across[...] = (
                tile_sum[...] + back_recv[...].astype(jnp.float32)
            ).astype(jnp.bfloat16)
        weight = weight_own if slot == OWN else weight_across
        folded = contract(pick_mom, greens[slot], ((1,), (0,)))
        folded = jnp.where(p == 0, folded[:, :half], folded[:, half:])
        joined = contract(split(folded), weight[...], ((1,), (0,)))
        joined = split(joined[:NMOM] + joined[NMOM:])
        picked = split(contract(pick_freq, greens[slot], ((1,), (0,))))
        value = contract(joined, picked[:LANES], ((1,), (1,)))
        value = (value[:NMOM] + value[NMOM:]
                 + contract(joined[:NMOM], picked[LANES:], ((1,), (1,))))
        cells_ref[...] = value if slot == OWN else cells_ref[...] + value

    def owner(i):
        to = lax.rem(me + i, count)
        return remote(sig_send.at[to], sig_recv.at[i - 1], s_send.at[0], s_recv.at[0],
                      (to // n_pair, lax.rem(to, n_pair)))

    def sigma():
        value_cells = cells_ref[...]
        rows_d = lax.broadcasted_iota(jnp.int32, (count, NMOM), 0)
        cols_m = lax.broadcasted_iota(jnp.int32, (count, NMOM), 1)
        spread = jnp.zeros((count, LANES), jnp.float32)
        if own_cells >= NFREQ:
            for k in range(folds):
                value = value_cells[k * count:(k + 1) * count, :]
                spread = spread + (pltpu.roll(value, NFREQ * k, 1) if k else value)
        else:
            group = NFREQ // own_cells
            for k in range(group):
                pick = (rows_d == cols_m * group + k).astype(jnp.float32)
                value = contract(pick, value_cells, ((1,), (0,)), lax.Precision.HIGHEST)
                spread = spread + (pltpu.roll(value, LANES - own_cells * k, 1) if k else value)
        factor = 1.0 / math.sqrt(5.0 * n_tiles * n_blk * states * states / (NMOM * NFREQ))
        sig_send[...] = (spread * (factor * out_scale)).reshape(count, 1, LANES)

        if count <= 32:
            for i in range(1, count):
                owner(i).start()
        else:
            def send_cells(i, carry):
                owner(i).start()
                return carry

            lax.fori_loop(1, count, send_cells, 0)

    def compute_inner(slot, part):
        upper = greens[slot, own_rows, :]
        for t in (part,):
            inner[slot, pl.ds(t * half, half), :] = contract(
                upper, tiles[t], ((1,), (0,))).astype(jnp.bfloat16)

    started = set()
    pending = {(0, part): 5 for part in range(n_tiles)} | {(1, part): 7 for part in range(n_tiles)}

    def compute_chi(group, slot, part, k_half=None):
        rows = own_rows if group == 0 else rest_rows
        cols = pl.ds(0, states) if k_half is None else pl.ds(k_half * wide, wide)
        first = (group, part) not in started
        started.add((group, part))
        pending[group, part] -= 1
        last = pending[group, part] == 0
        for t in (part,):
            lines = pl.ds(t * half, half)
            value = contract(inner[slot, lines, cols], greens[slot, rows, cols], ((1,), (1,)))
            if not first:
                value = acc[group, lines, :] + value
            if last:
                out_ref[t, :, rows] = (value * out_scale).astype(jnp.bfloat16)
            else:
                acc[group, lines, :] = value

    def take_y(k):
        rows = chunk(p, k)
        exchange(k, p).wait_recv()
        greens[OWN, *rows] = (
            partial[*rows] + arrived[*rows].astype(jnp.float32)
        ).astype(jnp.bfloat16)
        to_across(k).start()
        to_peer(k).start()

    def take_x(k):
        to_across(k).wait_recv()
        if k < middle:
            to_along(k).start()
        else:
            @pl.when(jnp.logical_not(wrap_send))
            def _():
                to_along(k).start()

        @pl.when(forwards_across)
        def _():
            forward(ACROSS, k).start()

    def take_z(k):
        to_along(k).wait_recv()
        if k < middle:
            @pl.when(wrap_recv)
            def _():
                to_other(k).start()

        @pl.when(jnp.logical_not(forwards_across))
        def _():
            forward(RELAYED, k).start()

    waited = {"p": 0, "f": 0}

    def need(kind, k):
        if kind in waited:
            while waited[kind] <= k:
                at = waited[kind]
                (to_peer(at) if kind == "p" else forward(ACROSS, at)).wait_recv()
                waited[kind] += 1

    for task in plan(total, n_tiles):
        kind = task[0]
        if kind == "y":
            take_y(task[1])
        elif kind == "x":
            take_x(task[1])
            if passed < rounds - 1:
                take(passed)
                passed += 1
                give(passed)
        elif kind == "z":
            take_z(task[1])
        elif kind == "need":
            need(task[1], task[2])
        elif kind == "cells":
            cells(task[1])
        elif kind == "sigma":
            while passed < rounds - 1:
                take(passed)
                passed += 1
                give(passed)
            take(passed)
            sigma()
        elif kind == "inner":
            compute_inner(task[1], task[2])
        elif kind == "own":
            compute_chi(0, task[1], task[2])
        elif kind == "rest":
            compute_chi(1, task[1], task[3], None if task[1] < RELAYED else task[2])

    remote(sending, arrived, y_send.at[0], y_recv.at[0], other).wait_send()
    remote(greens.at[OWN], greens.at[ACROSS], x_send.at[0], x_recv.at[0], across).wait_send()
    remote(greens.at[OWN], greens.at[PEER], p_send.at[0], p_recv.at[0], peer).wait_send()
    remote(greens.at[ACROSS], greens.at[FORWARDED], f_send.at[0], f_recv.at[0], peer).wait_send()
    upper = pl.ds(0, half)
    remote(greens.at[ACROSS, upper], greens.at[RELAYED, upper], z_send.at[0], z_recv.at[0],
           along).wait_send()

    @pl.when(jnp.logical_not(wrap_send))
    def _():
        remote(greens.at[ACROSS, upper], greens.at[RELAYED, upper], z_send.at[1], z_recv.at[0],
               along).wait_send()

    @pl.when(wrap_recv)
    def _():
        remote(greens.at[RELAYED, upper], greens.at[RELAYED, upper], w_send.at[0], z_recv.at[0],
               other).wait_send()

    send_tiles().wait_send()
    send_back().wait_send()

    cell_block = remote(sig_send.at[pl.ds(0, count - 1)], sig_recv, s_send.at[0], s_recv.at[0], peer)
    cell_block.wait_send()
    cell_block.wait_recv()
    summed = jnp.sum(sig_recv[...], axis=0) + sig_send[me]
    sigma_ref[...] = summed[0, :own_cells]


def solution(mesh):
    n_blk, n_pair = mesh.shape["blk"], mesh.shape["pair"]
    count = n_blk * n_pair

    def per_device(vertex, left_phase, right_phase, tiles, orders, momentum, frequency):
        height, breadth = vertex.shape[1], vertex.shape[2]
        states = right_phase.shape[2]
        n_tiles = tiles.shape[0]
        half = states // n_pair
        sizes = (n_blk, n_pair, height, breadth, states, n_tiles)
        bf16, f32 = jnp.bfloat16, jnp.float32
        dma = pltpu.SemaphoreType.DMA
        chunks = n_pair * SPLIT * (half // SIZE)
        rounds = max(n_blk // 8 - 1, 0) + 2
        chi, cells = pl.pallas_call(
            lambda *refs: body(sizes, *refs),
            out_shape=(
                pltpu.VMEM((n_tiles, half, states), bf16),
                pltpu.VMEM((NMOM * NFREQ // count,), f32),
            ),
            in_specs=[pl.BlockSpec(memory_space=pltpu.HBM)] * 7,
            out_specs=(pl.BlockSpec(memory_space=pltpu.VMEM),) * 2,
            scratch_shapes=[
                pltpu.SMEM((1,), jnp.int32),
                pltpu.VMEM((1, states), jnp.int32),
                pltpu.VMEM((1, states), jnp.int32),
                dma((3,)),
                pltpu.VMEM((height, breadth), bf16),
                pltpu.VMEM((height, states), bf16),
                pltpu.VMEM((n_pair, half, height), bf16),
                pltpu.VMEM((SPLIT, breadth, states // SPLIT), bf16),
                pltpu.VMEM((n_tiles, states, states), bf16),
                pltpu.VMEM((SPLIT, height, states // SPLIT), bf16),
                pltpu.VMEM((states, states), f32),
                pltpu.VMEM((states, states), bf16),
                pltpu.VMEM((states, states), bf16),
                pltpu.VMEM((5, states, states), bf16),
                pltpu.VMEM((5, n_tiles * half, states), bf16),
                pltpu.VMEM((2, n_tiles * half, half), f32),
                pltpu.VMEM((half, states), f32),
            ] + [pltpu.VMEM((half, states), bf16)] * 6 + [
                pltpu.VMEM((NMOM, LANES), f32),
                pltpu.VMEM((count, 1, LANES), f32),
                pltpu.VMEM((count - 1, 1, LANES), f32),
                dma((SPLIT + PIECES + 3,)),
            ] + [dma((1,)), dma((chunks,))] * 2 + [dma((2,)), dma((chunks,))] + [dma((1,)), dma((chunks,))] * 2 + [
                dma((1,))] + [dma((2,))] * 2 + [dma((1,))] * 2 + [
                pltpu.SemaphoreType.REGULAR((rounds,))],
            compiler_params=pltpu.CompilerParams(
                collective_id=0, has_side_effects=True, vmem_limit_bytes=60 * 1024 * 1024
            ),
            name="measure_green",
        )(
            orders,
            momentum.reshape(1, states),
            frequency.reshape(1, states),
            vertex,
            left_phase,
            right_phase,
            tiles,
        )
        return chi, cells

    in_specs = (
        P("blk", "pair", None),
        P("blk", "pair", None),
        P("blk", None, None),
        P("blk", None, None),
        P("blk"),
        P(),
        P(),
    )
    out_specs = (P("blk", "pair", None), P(("blk", "pair")))
    return jax.shard_map(
        per_device, mesh=mesh, in_specs=in_specs, out_specs=out_specs, check_vma=False
    )
```

```python
import math

import jax
import jax.numpy as jnp
from jax import lax
from jax.experimental import pallas as pl
from jax.experimental.pallas import tpu as pltpu
from jax.sharding import PartitionSpec as P

NMOM = 64
NFREQ = 32
LANES = 128
SIZE = 128
SPLIT = 2
PIECES = 4
MESH = pl.DeviceIdType.MESH
OWN, PEER, ACROSS, RELAYED, FORWARDED = range(5)

FIRST, HOP, NEAR, LATE, LAST, STEP = 8.2, 1.9, 1.0, 3.0, 4.0, 1.41
INNER, CHI = 0.2, 0.11


def contract(a, b, dims, precision=None):
    return lax.dot_general(
        a, b, (dims, ((), ())), preferred_element_type=jnp.float32, precision=precision
    )


def plan(count, parts):
    step = STEP * 8 / count
    half = count // 2
    quarter = count // 4
    arrive = {}
    for k in range(count):
        y = FIRST + step * (k + 1)
        arrive["y", k] = y
        arrive["x", k] = y + step + HOP
        arrive["z", k] = y + 2 * (step + HOP) + (LATE if k < half else max(LAST - LATE, 0.0))
        arrive["p", k] = y + NEAR
    for k in range(half, count):
        arrive["z", k] = max(arrive["z", k], arrive["z", k - half] + step + HOP)
    for k in range(count):
        arrive["f", k] = arrive["z", k] + NEAR
    source = {OWN: "y", PEER: "p", ACROSS: "x", RELAYED: "z", FORWARDED: "f"}
    jobs = []
    for slot in range(5):
        s = source[slot]
        for part in range(parts):
            jobs.append((arrive[s, half - 1], INNER, ("inner", slot, part), [(s, half - 1)], []))
        for part in range(parts):
            jobs.append((arrive[s, half - 1], CHI, ("own", slot, part), [(s, half - 1)],
                         [("inner", slot, part)]))
        for h in range(2):
            k = half + quarter * (h + 1) - 1
            if slot < RELAYED and h == 0:
                continue
            for part in range(parts):
                length = CHI if slot < RELAYED else CHI / 2
                jobs.append((arrive[s, k], length, ("rest", slot, h, part), [(s, k)],
                             [("inner", slot, part)]))
    jobs.append((arrive["y", count - 1], 0.3, ("cells", OWN), [("y", count - 1)], []))
    jobs.append((arrive["x", count - 1], 0.3, ("cells", ACROSS), [("x", count - 1)],
                 [("cells", OWN)]))
    jobs.append((arrive["x", count - 1], 0.3, ("sigma",), [("x", count - 1)], [("cells", ACROSS)]))
    urgent = {"cells": 1, "sigma": 1, "inner": 2, "own": 3, "rest": 3}
    waits = sorted((t, key) for key, t in arrive.items() if key[0] in "yxz")
    order, done, now = [], set(), 0.0
    taken = set()
    while waits or jobs:
        if waits and waits[0][0] <= now + 0.05:
            t, key = waits.pop(0)
            now = max(now, t)
            order.append(key)
            taken.add(key)
            continue
        ready = [j for j in jobs if j[0] <= now and all(d in done for d in j[4])
                 and all(w in taken or w[0] in "pf" for w in j[3])]
        if ready:
            job = min(ready, key=lambda j: (urgent[j[2][0]], j[0]))
            jobs.remove(job)
            for w in job[3]:
                order.append(("need",) + w)
            order.append(job[2])
            done.add(job[2])
            now += job[1]
            continue
        times = [j[0] for j in jobs if j[0] > now] + ([waits[0][0]] if waits else [])
        now = min(times)
    return order


def body(sizes, order_hbm, mom_hbm, freq_hbm, vertex_hbm, left_hbm, right_hbm, tiles_hbm,
         out_ref, sigma_ref,
         order_ref, mom_ref, freq_ref, small_sem, vertex, left, turned, right, tiles, carried, partial, sending, arrived, greens, inner, acc,
         tile_sum, tile_send, tile_recv, back_send, back_recv, weight_own, weight_across,
         cells_ref, sig_send, sig_recv, load_sem, y_send, y_recv, x_send, x_recv, z_send, z_recv,
         p_send, p_recv, f_send, f_recv, w_send, t_send, t_recv, s_send, s_recv, token):
    n_blk, n_pair, height, breadth, states, n_tiles = sizes
    count = n_blk * n_pair
    half = states // n_pair
    b = lax.axis_index("blk")
    p = lax.axis_index("pair")
    me = b * n_pair + p
    chip = b // 2
    core = lax.rem(b, 2)
    odd = lax.rem(chip, 2)
    step = 1 - 2 * odd
    across = (lax.rem(b + 2 * step + n_blk, n_blk), p)
    along = (lax.rem(b + 4 * step + n_blk, n_blk), p)
    back = (lax.rem(b - 4 * step + n_blk, n_blk), p)
    peer = (b + 1 - 2 * core, p)
    other = (b, 1 - p)
    forwards_across = lax.rem(odd + core, 2) == 0
    low_end = b < 4
    high_end = b >= n_blk - 4
    even = odd == 0
    wrap_send = jnp.logical_or(jnp.logical_and(even, high_end),
                               jnp.logical_and(jnp.logical_not(even), low_end))
    wrap_recv = jnp.logical_or(jnp.logical_and(even, low_end),
                               jnp.logical_and(jnp.logical_not(even), high_end))

    barrier = pltpu.get_barrier_semaphore()

    def tell(semaphore, devices):
        for device in devices:
            pl.semaphore_signal(semaphore, inc=1, device_id=device, device_id_type=MESH)

    def tell_column(semaphore):
        tell(semaphore, (along, back))

    beside = 2
    tell(barrier, (other, across, peer))
    tell_column(barrier)

    pieces = PIECES
    block = height // pieces
    wide = states // SPLIT

    def load_right(h):
        cols = pl.ds(h * wide, wide)
        return pltpu.make_async_copy(right_hbm.at[0, :, cols], right.at[h], load_sem.at[h])

    small = [
        pltpu.make_async_copy(order_hbm, order_ref, small_sem.at[0]),
        pltpu.make_async_copy(mom_hbm, mom_ref, small_sem.at[1]),
        pltpu.make_async_copy(freq_hbm, freq_ref, small_sem.at[2]),
    ]
    load_left = pltpu.make_async_copy(left_hbm.at[0], left, load_sem.at[SPLIT + pieces])
    load_vertex = []
    for i in range(pieces):
        rows = pl.ds(i * block, block)
        load_vertex.append(
            pltpu.make_async_copy(vertex_hbm.at[0, rows], vertex.at[rows], load_sem.at[SPLIT + i]))
    own_rows = pl.ds(pl.multiple_of(p * half, half), half)
    rest_rows = pl.ds(pl.multiple_of((1 - p) * half, half), half)
    load_tiles = [
        pltpu.make_async_copy(tiles_hbm.at[:, rows], tiles.at[:, rows], load_sem.at[at])
        for rows, at in ((own_rows, SPLIT + 1 + pieces), (rest_rows, SPLIT + 2 + pieces))
    ]
    queue = list(load_vertex) + [load_right(h) for h in range(1, SPLIT)] + load_tiles[1:] + small[1:]

    def pump(number):
        for copy in queue[:number]:
            copy.start()
        del queue[:number]

    small[0].start()
    load_left.start()
    load_right(0).start()
    load_tiles[0].start()
    pump(2)

    scale = 1.0 / math.sqrt(breadth)
    per = half // SIZE
    total = n_pair * SPLIT * per
    middle = total // 2

    def chunk(which, k):
        group, h, i = k // (SPLIT * per), k // per % SPLIT, k % per
        start = lax.rem(which + group, n_pair) * half + i * SIZE
        return pl.ds(pl.multiple_of(start, SIZE), SIZE), pl.ds(h * wide, wide)

    def remote(src, dst, send, recv, device):
        return pltpu.make_async_remote_copy(src_ref=src, dst_ref=dst, send_sem=send, recv_sem=recv,
                                            device_id=device, device_id_type=MESH)

    def exchange(k, which):
        rows = chunk(which, k)
        return remote(sending.at[*rows], arrived.at[*rows], y_send.at[0], y_recv.at[k], other)

    def hop(source, target, k, send, recv, device):
        rows = chunk(p, k)
        return remote(greens.at[source, *rows], greens.at[target, *rows], send, recv, device)

    def to_across(k):
        return hop(OWN, ACROSS, k, x_send.at[0], x_recv.at[k], across)

    def to_peer(k):
        return hop(OWN, PEER, k, p_send.at[0], p_recv.at[k], peer)

    def to_along(k):
        return hop(ACROSS, RELAYED, k, z_send.at[k // middle], z_recv.at[k], along)

    def to_other(k):
        return hop(RELAYED, RELAYED, k, w_send.at[0], z_recv.at[k + middle], other)

    def forward(source, k):
        return hop(source, FORWARDED, k, f_send.at[0], f_recv.at[k], peer)

    def send_tiles():
        return remote(tile_send, tile_recv, t_send.at[0], t_recv.at[0], peer)

    def send_back():
        return remote(back_send, back_recv, t_send.at[1], t_recv.at[1], back)

    column = max(n_blk // 8 - 1, 0)
    rounds = column + 2

    def give(r):
        if r < column:
            tell_column(token.at[r])
        else:
            tell(token.at[r], (other, across, peer))

    def take(r):
        pl.semaphore_wait(token.at[r], beside if r < column else 3)

    def mask_right(h):
        def part(i, carry):
            rows = pl.ds(pl.multiple_of(i * 256, 256), 256)
            ids = i * 256 + lax.broadcasted_iota(jnp.int32, (256, wide), 0)
            right[h, rows, :] = jnp.where(ids < order, right[h, rows, :],
                                          jnp.zeros((), jnp.bfloat16))
            return carry

        lax.fori_loop(0, breadth // 256, part, 0)

    def carry_half(h):
        for i in range(pieces):
            rows = pl.ds(i * block, block)
            if h == 0:
                load_vertex[i].wait()
                pump(1)
            product = contract(vertex[rows, :], right[h], ((1,), (0,)))
            ids = p * height + i * block + lax.broadcasted_iota(jnp.int32, (block, wide), 0)
            carried[h, rows, :] = jnp.where(ids < order, product, 0.0).astype(jnp.bfloat16)
            if h == 0 and i % 2 == 1:
                first_block(i // 2)

    def first_block(i):
        rows = pl.ds(pl.multiple_of((1 - p) * half, half), half)
        depth = pl.ds(2 * i * block, 2 * block)
        product = contract(turned[0, :, depth], carried[0, depth, :], ((1,), (0,))) * scale
        if i > 0:
            product = partial[rows, pl.ds(0, wide)] + product
        partial[rows, pl.ds(0, wide)] = product
        if i == pieces // 2 - 1:
            sending[rows, pl.ds(0, wide)] = product.astype(jnp.bfloat16)

    def send_block(group, h):
        for i in range(per):
            exchange((group * SPLIT + h) * per + i, 1 - p).start()

    def partial_block(group, h):
        which = lax.rem(1 - p + group, n_pair)
        rows = pl.ds(pl.multiple_of(which * half, half), half)
        cols = pl.ds(h * wide, wide)
        product = contract(turned[group], carried[h], ((1,), (0,))) * scale
        partial[rows, cols] = product
        sending[rows, cols] = product.astype(jnp.bfloat16)
        send_block(group, h)

    def turn(group):
        which = lax.rem(1 - p + group, n_pair)
        cols = pl.ds(pl.multiple_of(which * half, half), half)
        turned[group] = left[:, cols].T

    out_scale = 1.0 / math.sqrt(states)
    pair_share = forwards_across.astype(jnp.float32)

    def tile_stage(stage):
        if stage == 0:
            value = tiles[0, own_rows, :].astype(jnp.float32)
            for t in range(1, n_tiles):
                value = value + tiles[t, own_rows, :].astype(jnp.float32)
            tile_sum[...] = value
            tile_send[...] = value.astype(jnp.bfloat16)
        else:
            send_tiles().wait_recv()
            mine = tile_sum[...]
            theirs = tile_recv[...].astype(jnp.float32)
            back_send[...] = (mine + (1.0 - pair_share) * theirs).astype(jnp.bfloat16)
            send_back().start()
            weight_own[...] = (mine + theirs).astype(jnp.bfloat16)
            tile_sum[...] = mine + pair_share * theirs

    small[0].wait()
    order = order_ref[0]
    load_left.wait()
    pump(1)
    turn(0)
    load_right(0).wait()
    pump(1)
    mask_right(0)
    load_tiles[0].wait()
    tile_stage(0)
    carry_half(0)
    pump(len(queue))
    pl.semaphore_wait(barrier, 3 + beside)
    send_block(0, 0)
    send_tiles().start()
    passed = 0
    give(passed)
    load_tiles[1].wait()
    for h in range(1, SPLIT):
        load_right(h).wait()
        mask_right(h)
        carry_half(h)
        partial_block(0, h)
    tile_stage(1)
    for group in range(1, n_pair):
        turn(group)
        for h in range(SPLIT):
            partial_block(group, h)
    for copy in small[1:]:
        copy.wait()

    own_cells = NMOM * NFREQ // count
    folds = max(own_cells // NFREQ, 1)
    ids_m = lax.broadcasted_iota(jnp.int32, (NMOM, states), 0)
    ids_m = lax.rem(ids_m, NMOM // folds) * folds + ids_m // (NMOM // folds)
    pick_mom = (ids_m == mom_ref[...]).astype(jnp.bfloat16)
    ids_f = lax.broadcasted_iota(jnp.int32, (LANES, states), 0)
    pick_freq = (ids_f == freq_ref[...]).astype(jnp.bfloat16)

    def split(value):
        high = value.astype(jnp.bfloat16)
        low = (value - high.astype(jnp.float32)).astype(jnp.bfloat16)
        return jnp.concatenate([high, low], axis=0)

    def cells(slot):
        if slot == ACROSS:
            send_back().wait_recv()
            weight_across[...] = (
                tile_sum[...] + back_recv[...].astype(jnp.float32)
            ).astype(jnp.bfloat16)
        weight = weight_own if slot == OWN else weight_across
        folded = contract(pick_mom, greens[slot], ((1,), (0,)))
        folded = jnp.where(p == 0, folded[:, :half], folded[:, half:])
        joined = contract(split(folded), weight[...], ((1,), (0,)))
        joined = split(joined[:NMOM] + joined[NMOM:])
        picked = split(contract(pick_freq, greens[slot], ((1,), (0,))))
        value = contract(joined, picked[:LANES], ((1,), (1,)))
        value = (value[:NMOM] + value[NMOM:]
                 + contract(joined[:NMOM], picked[LANES:], ((1,), (1,))))
        cells_ref[...] = value if slot == OWN else cells_ref[...] + value

    def owner(i):
        to = lax.rem(me + i, count)
        return remote(sig_send.at[to], sig_recv.at[i - 1], s_send.at[0], s_recv.at[0],
                      (to // n_pair, lax.rem(to, n_pair)))

    def sigma():
        value_cells = cells_ref[...]
        rows_d = lax.broadcasted_iota(jnp.int32, (count, NMOM), 0)
        cols_m = lax.broadcasted_iota(jnp.int32, (count, NMOM), 1)
        spread = jnp.zeros((count, LANES), jnp.float32)
        if own_cells >= NFREQ:
            for k in range(folds):
                value = value_cells[k * count:(k + 1) * count, :]
                spread = spread + (pltpu.roll(value, NFREQ * k, 1) if k else value)
        else:
            group = NFREQ // own_cells
            for k in range(group):
                pick = (rows_d == cols_m * group + k).astype(jnp.float32)
                value = contract(pick, value_cells, ((1,), (0,)), lax.Precision.HIGHEST)
                spread = spread + (pltpu.roll(value, LANES - own_cells * k, 1) if k else value)
        factor = 1.0 / math.sqrt(5.0 * n_tiles * n_blk * states * states / (NMOM * NFREQ))
        sig_send[...] = (spread * (factor * out_scale)).reshape(count, 1, LANES)

        if count <= 32:
            for i in range(1, count):
                owner(i).start()
        else:
            def send_cells(i, carry):
                owner(i).start()
                return carry

            lax.fori_loop(1, count, send_cells, 0)

    def compute_inner(slot, part):
        upper = greens[slot, own_rows, :]
        for t in (part,):
            inner[slot, pl.ds(t * half, half), :] = contract(
                upper, tiles[t], ((1,), (0,))).astype(jnp.bfloat16)

    started = set()
    pending = {(0, part): 5 for part in range(n_tiles)} | {(1, part): 7 for part in range(n_tiles)}

    def compute_chi(group, slot, part, k_half=None):
        rows = own_rows if group == 0 else rest_rows
        cols = pl.ds(0, states) if k_half is None else pl.ds(k_half * wide, wide)
        first = (group, part) not in started
        started.add((group, part))
        pending[group, part] -= 1
        last = pending[group, part] == 0
        for t in (part,):
            lines = pl.ds(t * half, half)
            value = contract(inner[slot, lines, cols], greens[slot, rows, cols], ((1,), (1,)))
            if not first:
                value = acc[group, lines, :] + value
            if last:
                out_ref[t, :, rows] = (value * out_scale).astype(jnp.bfloat16)
            else:
                acc[group, lines, :] = value

    def take_y(k):
        rows = chunk(p, k)
        exchange(k, p).wait_recv()
        greens[OWN, *rows] = (
            partial[*rows] + arrived[*rows].astype(jnp.float32)
        ).astype(jnp.bfloat16)
        to_across(k).start()
        to_peer(k).start()

    def take_x(k):
        to_across(k).wait_recv()
        if k < middle:
            to_along(k).start()
        else:
            @pl.when(jnp.logical_not(wrap_send))
            def _():
                to_along(k).start()

        @pl.when(forwards_across)
        def _():
            forward(ACROSS, k).start()

    def take_z(k):
        to_along(k).wait_recv()
        if k < middle:
            @pl.when(wrap_recv)
            def _():
                to_other(k).start()

        @pl.when(jnp.logical_not(forwards_across))
        def _():
            forward(RELAYED, k).start()

    waited = {"p": 0, "f": 0}

    def need(kind, k):
        if kind in waited:
            while waited[kind] <= k:
                at = waited[kind]
                (to_peer(at) if kind == "p" else forward(ACROSS, at)).wait_recv()
                waited[kind] += 1

    for task in plan(total, n_tiles):
        kind = task[0]
        if kind == "y":
            take_y(task[1])
        elif kind == "x":
            take_x(task[1])
            if passed < rounds - 1:
                take(passed)
                passed += 1
                give(passed)
        elif kind == "z":
            take_z(task[1])
        elif kind == "need":
            need(task[1], task[2])
        elif kind == "cells":
            cells(task[1])
        elif kind == "sigma":
            while passed < rounds - 1:
                take(passed)
                passed += 1
                give(passed)
            take(passed)
            sigma()
        elif kind == "inner":
            compute_inner(task[1], task[2])
        elif kind == "own":
            compute_chi(0, task[1], task[2])
        elif kind == "rest":
            compute_chi(1, task[1], task[3], None if task[1] < RELAYED else task[2])

    remote(sending, arrived, y_send.at[0], y_recv.at[0], other).wait_send()
    remote(greens.at[OWN], greens.at[ACROSS], x_send.at[0], x_recv.at[0], across).wait_send()
    remote(greens.at[OWN], greens.at[PEER], p_send.at[0], p_recv.at[0], peer).wait_send()
    remote(greens.at[ACROSS], greens.at[FORWARDED], f_send.at[0], f_recv.at[0], peer).wait_send()
    upper = pl.ds(0, half)
    remote(greens.at[ACROSS, upper], greens.at[RELAYED, upper], z_send.at[0], z_recv.at[0],
           along).wait_send()

    @pl.when(jnp.logical_not(wrap_send))
    def _():
        remote(greens.at[ACROSS, upper], greens.at[RELAYED, upper], z_send.at[1], z_recv.at[0],
               along).wait_send()

    @pl.when(wrap_recv)
    def _():
        remote(greens.at[RELAYED, upper], greens.at[RELAYED, upper], w_send.at[0], z_recv.at[0],
               other).wait_send()

    send_tiles().wait_send()
    send_back().wait_send()

    cell_block = remote(sig_send.at[pl.ds(0, count - 1)], sig_recv, s_send.at[0], s_recv.at[0], peer)
    cell_block.wait_send()
    cell_block.wait_recv()
    summed = jnp.sum(sig_recv[...], axis=0) + sig_send[me]
    sigma_ref[...] = summed[0, :own_cells]


def solution(mesh):
    n_blk, n_pair = mesh.shape["blk"], mesh.shape["pair"]
    count = n_blk * n_pair

    def per_device(vertex, left_phase, right_phase, tiles, orders, momentum, frequency):
        height, breadth = vertex.shape[1], vertex.shape[2]
        states = right_phase.shape[2]
        n_tiles = tiles.shape[0]
        half = states // n_pair
        sizes = (n_blk, n_pair, height, breadth, states, n_tiles)
        bf16, f32 = jnp.bfloat16, jnp.float32
        dma = pltpu.SemaphoreType.DMA
        chunks = n_pair * SPLIT * (half // SIZE)
        rounds = max(n_blk // 8 - 1, 0) + 2
        chi, cells = pl.pallas_call(
            lambda *refs: body(sizes, *refs),
            out_shape=(
                pltpu.VMEM((n_tiles, half, states), bf16),
                pltpu.VMEM((NMOM * NFREQ // count,), f32),
            ),
            in_specs=[pl.BlockSpec(memory_space=pltpu.HBM)] * 7,
            out_specs=(pl.BlockSpec(memory_space=pltpu.VMEM),) * 2,
            scratch_shapes=[
                pltpu.SMEM((1,), jnp.int32),
                pltpu.VMEM((1, states), jnp.int32),
                pltpu.VMEM((1, states), jnp.int32),
                dma((3,)),
                pltpu.VMEM((height, breadth), bf16),
                pltpu.VMEM((height, states), bf16),
                pltpu.VMEM((n_pair, half, height), bf16),
                pltpu.VMEM((SPLIT, breadth, states // SPLIT), bf16),
                pltpu.VMEM((n_tiles, states, states), bf16),
                pltpu.VMEM((SPLIT, height, states // SPLIT), bf16),
                pltpu.VMEM((states, states), f32),
                pltpu.VMEM((states, states), bf16),
                pltpu.VMEM((states, states), bf16),
                pltpu.VMEM((5, states, states), bf16),
                pltpu.VMEM((5, n_tiles * half, states), bf16),
                pltpu.VMEM((2, n_tiles * half, half), f32),
                pltpu.VMEM((half, states), f32),
            ] + [pltpu.VMEM((half, states), bf16)] * 6 + [
                pltpu.VMEM((NMOM, LANES), f32),
                pltpu.VMEM((count, 1, LANES), f32),
                pltpu.VMEM((count - 1, 1, LANES), f32),
                dma((SPLIT + PIECES + 3,)),
            ] + [dma((1,)), dma((chunks,))] * 2 + [dma((2,)), dma((chunks,))] + [dma((1,)), dma((chunks,))] * 2 + [
                dma((1,))] + [dma((2,))] * 2 + [dma((1,))] * 2 + [
                pltpu.SemaphoreType.REGULAR((rounds,))],
            compiler_params=pltpu.CompilerParams(
                collective_id=0, has_side_effects=True, vmem_limit_bytes=60 * 1024 * 1024
            ),
            name="measure_green",
        )(
            orders,
            momentum.reshape(1, states),
            frequency.reshape(1, states),
            vertex,
            left_phase,
            right_phase,
            tiles,
        )
        return chi, cells

    in_specs = (
        P("blk", "pair", None),
        P("blk", "pair", None),
        P("blk", None, None),
        P("blk", None, None),
        P("blk"),
        P(),
        P(),
    )
    out_specs = (P("blk", "pair", None), P(("blk", "pair")))
    return jax.shard_map(
        per_device, mesh=mesh, in_specs=in_specs, out_specs=out_specs, check_vma=False
    )
```
